32 devices in a mesh: dp: 1, sp: 32 (over x, y, z, core).
Axes of the slice: x: 2, y: 2, z: 4, core: 2. Of those that a mesh axis runs over, the one named last changes fastest.
Arguments:
- x: bfloat16 [8192, 2048], P(('dp', 'sp'))
- gain: bfloat16 [2048], replicated
- wq: bfloat16 [2048, 2048], P('sp')
- wk: bfloat16 [2048, 256], P('sp')
- wv: bfloat16 [2048, 256], P('sp')
- wo: bfloat16 [2048, 2048], P('sp')
Outputs:
- output: bfloat16 [8192, 2048], P(('dp', 'sp'))
All inputs are finite; a program needn't handle non-finite values.
Results may differ from the reference program's by a relative error of at most 0.012.
Values are sent between devices in bfloat16 or wider.
A program may use at most 2 GiB of HBM per device.

```python
import jax
import jax.numpy as jnp
from jax import lax

ROWS = 8192
D = 2048
HEADS = 8
KV_HEADS = 1
HEAD = 256
THETA = 10000


def setup_inputs(seed: int = 0, part: int = 0) -> dict:
    kx, kn, kq, kk, kv, ko = jax.random.split(jax.random.key(seed), 6)

    def weights(key, rows, columns):
        return jax.random.normal(key, (rows, columns), jnp.float32) * rows**-0.5

    drawn = {
        "x": jax.random.normal(jax.random.fold_in(kx, part), (ROWS, D), jnp.float32),
        "gain": 1 + 0.1 * jax.random.normal(kn, (D,), jnp.float32),
        "wq": 2 * weights(kq, D, HEADS * HEAD),
        "wk": 2 * weights(kk, D, KV_HEADS * HEAD),
        "wv": 4 * weights(kv, D, KV_HEADS * HEAD),
        "wo": weights(ko, HEADS * HEAD, D),
    }
    return {k: v.astype(jnp.bfloat16) for k, v in drawn.items()}


def normed(x, gain):
    wide = x.astype(jnp.float32)
    scale = lax.rsqrt(jnp.mean(wide * wide, -1, keepdims=True) + 1e-6)
    return (wide * scale * gain.astype(jnp.float32)).astype(jnp.bfloat16)


def turned(t, place, theta):
    half = t.shape[-1] // 2
    angle = place.astype(jnp.float32)[:, None] * theta ** (-jnp.arange(half, dtype=jnp.float32) / half)
    cos, sin = jnp.cos(angle)[:, None], jnp.sin(angle)[:, None]
    a, b = t[..., :half].astype(jnp.float32), t[..., half:].astype(jnp.float32)
    return jnp.concatenate([a * cos - b * sin, b * cos + a * sin], -1).astype(jnp.bfloat16)


def matmul(a, w):
    return jnp.dot(a, w, preferred_element_type=jnp.float32).astype(jnp.bfloat16)


def einsum(form, a, b):
    return jnp.einsum(form, a.astype(jnp.float32), b.astype(jnp.float32))


def attention(q, k, v):
    scores = einsum("tgsd,ugd->gstu", q, k) * q.shape[-1] ** -0.5
    token = jnp.arange(q.shape[0])
    scores = jnp.where(token[:, None] >= token, scores, -jnp.inf)
    weights = jax.nn.softmax(scores, -1).astype(jnp.bfloat16)
    return einsum("gstu,ugd->tgsd", weights, v).astype(jnp.bfloat16)


def reference(x, gain, wq, wk, wv, wo):
    a, place = normed(x, gain), jnp.arange(ROWS)
    q = turned(matmul(a, wq).reshape(ROWS, HEADS, HEAD), place, THETA).reshape(ROWS, KV_HEADS, -1, HEAD)
    k = turned(matmul(a, wk).reshape(ROWS, KV_HEADS, HEAD), place, THETA)
    v = matmul(a, wv).reshape(ROWS, KV_HEADS, HEAD)
    seen = attention(q, k, v).reshape(ROWS, HEADS * HEAD)
    return (x.astype(jnp.float32) + jnp.dot(seen, wo, preferred_element_type=jnp.float32)).astype(jnp.bfloat16)
```

```python
import functools

import jax
import jax.numpy as jnp
import numpy as np
from jax import lax
from jax.experimental import pallas as pl
from jax.experimental.pallas import tpu as pltpu
from jax.sharding import PartitionSpec as P

HEAD = 256
THETA = 10000
LOG2E = 1.4426950408889634
HIDDEN = -1e30
MESH = pl.DeviceIdType.MESH
F32, BF16 = jnp.float32, jnp.bfloat16
WKV, WQ, KV, WO = range(4)

STAGES = (
    ((0, 0),),
    ((1, 0), (0, 1), (0, 2)),
    ((2, 0), (1, 1), (1, 2), (0, 3)),
    ((3, 0), (2, 1), (2, 2), (1, 3)),
    ((3, 1), (3, 2), (2, 3)),
    ((3, 3),),
)


def dot(a, b):
    return jnp.dot(a, b, preferred_element_type=F32)


def kernel(x_ref, gain_ref, freq_ref, wq_ref, wk_ref, wv_ref, wo_ref, out_ref,
           wqb, wob, wkvb, kvb, a_s, qt_s, mix_s, top_s, seen_s, cos_s, sin_s,
           local_sem, up_s, down_s, z_r, x_s, x_r, y_s, y_r, ha_s, ha_r, hb_s, hb_r, p_s, p_r):
    me = lax.axis_index("sp")
    core, chip = lax.rem(me, 2), lax.div(me, 2)
    z, y, x = lax.rem(chip, 4), lax.rem(lax.div(chip, 4), 2), lax.div(chip, 8)
    ranks = (z, z + 1 - 2 * lax.rem(z, 2), jnp.where(z >= 2, 1, 2), jnp.where(z >= 2, 0, 3))
    columns = ((x * 2 + y) * 4, (x * 2 + 1 - y) * 4, ((1 - x) * 2 + y) * 4, ((1 - x) * 2 + 1 - y) * 4)
    above, below, partner = me + 2, me - 2, me + 1 - 2 * core
    x_peer, y_peer = columns[2] * 2 + z * 2 + core, columns[1] * 2 + z * 2 + core
    bufs = (wkvb, wqb, kvb, wob)

    def remote(src, send_sem, recv_sem, to):
        return pltpu.make_async_remote_copy(src_ref=src, dst_ref=src, send_sem=send_sem, recv_sem=recv_sem, device_id={"sp": to}, device_id_type=MESH)

    def given(when, do):
        if when is None:
            do()
        else:
            pl.when(when)(do)

    def arrived(ref, recv_sem):
        pltpu.make_async_remote_copy(src_ref=ref, dst_ref=ref, send_sem=recv_sem, recv_sem=recv_sem, device_id={"sp": partner}, device_id_type=MESH).wait_recv()

    def whole(u, r, q, c):
        return bufs[u].at[columns[q] + ranks[r], c]

    def half(u, r, q, c, n):
        rows = bufs[u].shape[2] // 2
        return bufs[u].at[columns[q] + ranks[r], c, pl.ds(n * rows, rows)]

    def sends(u, r, q):
        ref = whole(u, r, q, core)
        copies = [(remote(ref, p_s.at[u, 4 * q + r], p_r.at[u, 4 * q + r], partner), None)]
        if q == 0:
            at = ranks[r]
            copies = [
                (remote(ref, up_s.at[u, r], z_r.at[u, at], above), (at <= z) & (z < 3)),
                (remote(ref, down_s.at[u, r], z_r.at[u, at], below), (at >= z) & (z > 0)),
                (remote(ref, x_s.at[u, r], x_r.at[u, r], x_peer), None),
                (remote(ref, y_s.at[u, r], y_r.at[u, r], y_peer), None),
            ] + copies
        elif q == 1:
            copies = [(remote(half(u, r, q, core, 1), hb_s.at[u, r], hb_r.at[u, r], x_peer), None)] + copies
        elif q == 2:
            copies = [(remote(half(u, r, q, core, 0), ha_s.at[u, r], ha_r.at[u, r], y_peer), None)] + copies
        return copies

    def event(u, r, q):
        if q == 0 and r:
            arrived(whole(u, r, q, core), z_r.at[u, ranks[r]])
        elif q == 1:
            arrived(whole(u, r, q, core), y_r.at[u, r])
        elif q == 2:
            arrived(whole(u, r, q, core), x_r.at[u, r])
        elif q == 3:
            arrived(half(u, r, q, core, 0), ha_r.at[u, r])
            arrived(half(u, r, q, core, 1), hb_r.at[u, r])
        for copy, when in sends(u, r, q):
            given(when, copy.start)

    def stage(u, n):
        for r, q in STAGES[n]:
            event(u, r, q)

    def other(u, r, q):
        arrived(whole(u, r, q, 1 - core), p_r.at[u, 4 * q + r])

    def others(u):
        for q in range(4):
            for r in range(4):
                other(u, r, q)

    own = [
        pltpu.make_async_copy(wk_ref, wkvb.at[chip, core, :, pl.ds(0, HEAD)], local_sem.at[0]),
        pltpu.make_async_copy(wv_ref, wkvb.at[chip, core, :, pl.ds(HEAD, HEAD)], local_sem.at[1]),
        pltpu.make_async_copy(wq_ref, wqb.at[chip, core], local_sem.at[2]),
        pltpu.make_async_copy(wo_ref, wob.at[chip, core], local_sem.at[3]),
    ]
    for copy in own:
        copy.start()

    barrier = pltpu.get_barrier_semaphore()

    def greet(to):
        pl.semaphore_signal(barrier, inc=1, device_id={"sp": to}, device_id_type=MESH)

    for to in (x_peer, y_peer, partner):
        greet(to)
    pl.when(z < 3)(lambda: greet(above))
    pl.when(z > 0)(lambda: greet(below))
    pl.semaphore_wait(barrier, jnp.where((z > 0) & (z < 3), 5, 4))

    own[0].wait()
    own[1].wait()
    stage(WKV, 0)
    own[2].wait()
    stage(WQ, 0)

    rows = x_ref.shape[0]

    @pl.loop(0, rows // 64)
    def _(n):
        here = pl.ds(n * 64, 64)
        wide = x_ref[here, :].astype(F32)
        scale = lax.rsqrt(jnp.mean(wide * wide, -1, keepdims=True) + 1e-6)
        a_s[here, :] = (wide * scale * gain_ref[...].astype(F32)).astype(BF16)

    place = (me * rows + lax.broadcasted_iota(jnp.int32, (rows, HEAD // 2), 0)).astype(F32)
    angle = place * freq_ref[...]
    cos_s[...] = jnp.cos(angle)
    sin_s[...] = jnp.sin(angle)

    def turned(t):
        t = t.astype(BF16).astype(F32)
        a, b, cos, sin = t[:, : HEAD // 2], t[:, HEAD // 2 :], cos_s[...], sin_s[...]
        return jnp.concatenate([a * cos - b * sin, b * cos + a * sin], -1)

    for n in range(1, 5):
        stage(WKV, n)
        stage(WQ, n)
    stage(WKV, 5)
    others(WKV)

    kv = dot(a_s[...], wkvb[...].reshape(-1, 2 * HEAD))
    kvb[chip, core, 0:HEAD, :] = turned(kv[:, :HEAD]).astype(BF16)
    kvb[chip, core, HEAD:, :] = kv[:, HEAD:].astype(BF16).astype(F32).T.astype(BF16)
    stage(KV, 0)
    stage(WQ, 5)
    others(WQ)

    heads = wqb.shape[3] // HEAD

    @pl.loop(0, heads)
    def _(h):
        cols = pl.ds(pl.multiple_of(h * HEAD, HEAD), HEAD)
        q = dot(a_s[...], wqb[:, :, :, cols].reshape(-1, HEAD))
        qt_s[:, cols] = turned(q).T.astype(BF16)

    e = HEAD**-0.5 * LOG2E
    width = qt_s.shape[1]
    strip = 512
    strips = range(0, width, strip)
    keys = 2 * rows
    ones = jnp.ones((8, keys), BF16)

    def step(at, masked):
        k = kvb[at, :, 0:HEAD, :].reshape(keys, HEAD)
        v = jnp.concatenate([kvb[at, 0, HEAD:, :], kvb[at, 1, HEAD:, :]], axis=1)
        v = jnp.concatenate([v, ones], axis=0)
        scores = [dot(k, qt_s[:, n : n + strip]) for n in strips]
        weights, keeps = [], []
        for n, s in zip(strips, scores):
            if masked:
                ahead = lax.rem(lax.broadcasted_iota(jnp.int32, s.shape, 1), rows) - lax.broadcasted_iota(jnp.int32, s.shape, 0)
                s = jnp.where(ahead >= -rows * core, s, HIDDEN)
                top = s.max(axis=0, keepdims=True)
            else:
                old = top_s[0:1, n : n + strip]
                top = jnp.maximum(old, s.max(axis=0, keepdims=True))
                keeps.append(jnp.exp2((old - top) * e))
            top_s[0:1, n : n + strip] = top
            weights.append(jnp.exp2((s - top) * e).astype(BF16))
        for i, n in enumerate(strips):
            add = dot(v, weights[i])
            mix_s[:, n : n + strip] = add if masked else mix_s[:, n : n + strip] * keeps[i] + add

    stage(KV, 1)
    other(KV, 0, 0)
    step(chip, True)

    @pl.loop(1, 16)
    def _(i):
        def at(n, *todo):
            @pl.when(i == n)
            def _():
                for do in todo:
                    do()

        for r in range(4):
            for q in range(4):
                n = 4 * r + q
                todo = []
                if n == 3:
                    todo.append(lambda: stage(KV, 2))
                if n == 4:
                    todo.append(lambda: stage(KV, 3))
                if n == 5:
                    todo.append(own[3].wait)
                    todo.append(lambda: stage(WO, 0))
                if n == 8:
                    todo.append(lambda: stage(KV, 4))
                if n == 9:
                    todo.append(lambda: stage(WO, 1))
                if n == 11:
                    todo.append(lambda: stage(KV, 5))
                if n == 13:
                    todo.append(lambda: stage(WO, 2))
                if n:
                    todo.append(functools.partial(other, KV, r, q))
                    at(n, *todo)

        r, q = lax.div(i, 4), lax.rem(i, 4)
        rank = jnp.where(r == 0, ranks[0], jnp.where(r == 1, ranks[1], jnp.where(r == 2, ranks[2], ranks[3])))
        column = jnp.where(q == 0, columns[0], jnp.where(q == 1, columns[1], jnp.where(q == 2, columns[2], columns[3])))
        block = column + rank

        @pl.when(block < chip)
        def _():
            step(block, False)

    stage(WO, 3)

    @pl.loop(0, heads)
    def _(h):
        cols = pl.ds(pl.multiple_of(h * HEAD, HEAD), HEAD)
        o = mix_s[0:HEAD, cols] * (1 / mix_s[HEAD : HEAD + 1, cols])
        seen_s[:, cols] = o.T.astype(BF16)

    stage(WO, 4)
    stage(WO, 5)
    others(WO)

    @pl.loop(0, out_ref.shape[1] // HEAD)
    def _(n):
        cols = pl.ds(pl.multiple_of(n * HEAD, HEAD), HEAD)
        got = dot(seen_s[...], wob[:, :, :, cols].reshape(-1, HEAD))
        out_ref[:, cols] = (x_ref[:, cols].astype(F32) + got).astype(BF16)

    for u in range(4):
        for r in range(4):
            for q in range(4):
                for copy, when in sends(u, r, q):
                    given(when, copy.wait_send)


def solution(mesh):
    half = HEAD // 2
    freq = (float(THETA) ** (-np.arange(half, dtype=np.float64) / half)).astype(np.float32)[None]

    def step(x, gain, wq, wk, wv, wo):
        rows, wide = x.shape
        deep, width = wq.shape
        vmem, hbm = pl.BlockSpec(memory_space=pltpu.VMEM), pl.BlockSpec(memory_space=pltpu.HBM)
        dma = pltpu.SemaphoreType.DMA
        return pl.pallas_call(
            kernel,
            out_shape=jax.ShapeDtypeStruct((rows, wide), BF16),
            in_specs=[vmem] * 3 + [hbm] * 4,
            out_specs=vmem,
            scratch_shapes=[
                pltpu.VMEM((16, 2, deep, width), BF16),
                pltpu.VMEM((16, 2, deep, wide), BF16),
                pltpu.VMEM((16, 2, deep, 2 * HEAD), BF16),
                pltpu.VMEM((16, 2, 2 * HEAD, HEAD), BF16),
                pltpu.VMEM((rows, wide), BF16),
                pltpu.VMEM((HEAD, width), BF16),
                pltpu.VMEM((HEAD + 8, width), F32),
                pltpu.VMEM((8, width), F32),
                pltpu.VMEM((rows, width), BF16),
                pltpu.VMEM((rows, half), F32),
                pltpu.VMEM((rows, half), F32),
                dma((4,)),
                *[dma((4, 4))] * 11,
                *[dma((4, 16))] * 2,
            ],
            compiler_params=pltpu.CompilerParams(collective_id=0, has_side_effects=True, vmem_limit_bytes=63 * 2**20),
        )(x, gain[None], jnp.asarray(freq), wq, wk, wv, wo)

    tokens, whole = P(("dp", "sp"), None), P("sp", None)
    return jax.shard_map(step, mesh=mesh, in_specs=(tokens, P(None), whole, whole, whole, whole), out_specs=tokens, check_vma=False)
```

```python
import functools

import jax
import jax.numpy as jnp
import numpy as np
from jax import lax
from jax.experimental import pallas as pl
from jax.experimental.pallas import tpu as pltpu
from jax.sharding import PartitionSpec as P

HEAD = 256
THETA = 10000
LOG2E = 1.4426950408889634
HIDDEN = -1e30
MESH = pl.DeviceIdType.MESH
F32, BF16 = jnp.float32, jnp.bfloat16
WKV, WQ, KV, WO = range(4)

STAGES = (
    ((0, 0),),
    ((1, 0), (0, 1), (0, 2)),
    ((2, 0), (1, 1), (1, 2), (0, 3)),
    ((3, 0), (2, 1), (2, 2), (1, 3)),
    ((3, 1), (3, 2), (2, 3)),
    ((3, 3),),
)
MAIN, A, B, LATE, LATE_A, LATE_B = range(6)
CUTS = {
    WKV: (1, ((0, 512), (0, 256), (256, 256), None, None, None)),
    WQ: (1, ((0, 1536), (0, 768), (768, 768), (1536, 512), (1536, 256), (1792, 256))),
    KV: (0, ((0, 384), (0, 192), (192, 192), (384, 128), (384, 64), (448, 64))),
    WO: (1, ((0, 1536), (0, 768), (768, 768), (1536, 512), (1536, 256), (1792, 256))),
}


WORK = {3: ((KV, 3),), 4: ((WO, 0),), 7: ((KV, 4),), 8: ((WO, 1),), 10: ((WO, 2),), 11: ((KV, 5),), 13: ((WO, 3),)}


def dot(a, b):
    return jnp.dot(a, b, preferred_element_type=F32)


def kernel(x_ref, gain_ref, freq_ref, wq_ref, wk_ref, wv_ref, wo_ref, out_ref,
           wqb, wob, wkvb, kvb, a_s, qt_s, mix_s, top_s, seen_s, cos_s, sin_s,
           local_sem, up_s, down_s, z_r, x_s, x_r, y_s, y_r, ha_s, ha_r, hb_s, hb_r, p_s, p_r,
           late_s, late_r, late_up_s, late_down_s, late_z_r, late_p_s, late_p_r):
    me = lax.axis_index("sp")
    core, chip = lax.rem(me, 2), lax.div(me, 2)
    z, y, x = lax.rem(chip, 4), lax.rem(lax.div(chip, 4), 2), lax.div(chip, 8)
    ranks = (z, z + 1 - 2 * lax.rem(z, 2), jnp.where(z >= 2, 1, 2), jnp.where(z >= 2, 0, 3))
    columns = (x * 2 + y, x * 2 + 1 - y, (1 - x) * 2 + y, (1 - x) * 2 + 1 - y)
    above, below, partner = me + 2, me - 2, me + 1 - 2 * core
    x_peer, y_peer = columns[2] * 8 + z * 2 + core, columns[1] * 8 + z * 2 + core
    bufs = (wkvb, wqb, kvb, wob)

    def remote(src, send_sem, recv_sem, to):
        return pltpu.make_async_remote_copy(src_ref=src, dst_ref=src, send_sem=send_sem, recv_sem=recv_sem, device_id={"sp": to}, device_id_type=MESH)

    def given(when, do):
        if when is None:
            do()
        else:
            pl.when(when)(do)

    def arrived(ref, recv_sem):
        pltpu.make_async_remote_copy(src_ref=ref, dst_ref=ref, send_sem=recv_sem, recv_sem=recv_sem, device_id={"sp": partner}, device_id_type=MESH).wait_recv()

    def piece(u, r, q, c, which):
        axis, cuts = CUTS[u]
        start, size = cuts[which]
        column = slice(None) if q is None else columns[q]
        here = pl.ds(start, size)
        return bufs[u].at[column, ranks[r], c, here] if axis == 0 else bufs[u].at[column, ranks[r], c, :, here]

    def sends(u, r, q):
        ref = piece(u, r, q, core, MAIN)
        copies = [(remote(ref, p_s.at[u, 4 * q + r], p_r.at[u, 4 * q + r], partner), None)]
        if q == 0:
            at = ranks[r]
            copies = [
                (remote(ref, up_s.at[u, r], z_r.at[u, at], above), (at <= z) & (z < 3)),
                (remote(ref, down_s.at[u, r], z_r.at[u, at], below), (at >= z) & (z > 0)),
                (remote(ref, x_s.at[u, r], x_r.at[u, r], x_peer), None),
                (remote(ref, y_s.at[u, r], y_r.at[u, r], y_peer), None),
            ] + copies
        elif q == 1:
            copies = [(remote(piece(u, r, q, core, B), hb_s.at[u, r], hb_r.at[u, r], x_peer), None)] + copies
        elif q == 2:
            copies = [(remote(piece(u, r, q, core, A), ha_s.at[u, r], ha_r.at[u, r], y_peer), None)] + copies
        return copies

    def event(u, r, q):
        if q == 0 and r:
            arrived(piece(u, r, q, core, MAIN), z_r.at[u, ranks[r]])
        elif q == 1:
            arrived(piece(u, r, q, core, MAIN), y_r.at[u, r])
        elif q == 2:
            arrived(piece(u, r, q, core, MAIN), x_r.at[u, r])
        elif q == 3:
            arrived(piece(u, r, q, core, A), ha_r.at[u, r])
            arrived(piece(u, r, q, core, B), hb_r.at[u, r])
        for copy, when in sends(u, r, q):
            given(when, copy.start)

    def late_sends(u, n):
        if n == 0:
            ref = piece(u, 0, 0, core, LATE)
            return [(remote(ref, late_s.at[u, 0], late_r.at[u, 0], x_peer), None), (remote(ref, late_s.at[u, 1], late_r.at[u, 1], y_peer), None)]
        if n == 1:
            return [
                (remote(piece(u, 0, 2, core, LATE_A), late_s.at[u, 2], late_r.at[u, 2], y_peer), None),
                (remote(piece(u, 0, 1, core, LATE_B), late_s.at[u, 3], late_r.at[u, 3], x_peer), None),
            ]
        r = n - 2
        at, ref = ranks[r], piece(u, r, None, core, LATE)
        return [
            (remote(ref, late_up_s.at[u, r], late_z_r.at[u, at], above), (at <= z) & (z < 3)),
            (remote(ref, late_down_s.at[u, r], late_z_r.at[u, at], below), (at >= z) & (z > 0)),
            (remote(ref, late_p_s.at[u, r], late_p_r.at[u, r], partner), None),
        ]

    def late_event(u, n):
        if n == 1:
            arrived(piece(u, 0, 2, core, LATE), late_r.at[u, 0])
            arrived(piece(u, 0, 1, core, LATE), late_r.at[u, 1])
        elif n == 2:
            arrived(piece(u, 0, 3, core, LATE_A), late_r.at[u, 2])
            arrived(piece(u, 0, 3, core, LATE_B), late_r.at[u, 3])
        elif n > 2:
            arrived(piece(u, n - 2, None, core, LATE), late_z_r.at[u, ranks[n - 2]])
        for copy, when in late_sends(u, n):
            given(when, copy.start)

    def stage(u, n):
        if u != WKV:
            late_event(u, n)
        for r, q in STAGES[n]:
            event(u, r, q)

    def other(u, r, q):
        arrived(piece(u, r, q, 1 - core, MAIN), p_r.at[u, 4 * q + r])
        if u != WKV and q == 0:
            arrived(piece(u, r, None, 1 - core, LATE), late_p_r.at[u, r])

    def others(u):
        for r in range(4):
            for q in range(4):
                other(u, r, q)

    own = [
        pltpu.make_async_copy(wk_ref, wkvb.at[columns[0], z, core, :, pl.ds(0, HEAD)], local_sem.at[0]),
        pltpu.make_async_copy(wv_ref, wkvb.at[columns[0], z, core, :, pl.ds(HEAD, HEAD)], local_sem.at[1]),
        pltpu.make_async_copy(wq_ref, wqb.at[columns[0], z, core], local_sem.at[2]),
        pltpu.make_async_copy(wo_ref, wob.at[columns[0], z, core], local_sem.at[3]),
    ]
    for copy in own:
        copy.start()

    barrier = pltpu.get_barrier_semaphore()

    def greet(to):
        pl.semaphore_signal(barrier, inc=1, device_id={"sp": to}, device_id_type=MESH)

    for to in (x_peer, y_peer, partner):
        greet(to)
    pl.when(z < 3)(lambda: greet(above))
    pl.when(z > 0)(lambda: greet(below))
    pl.semaphore_wait(barrier, jnp.where((z > 0) & (z < 3), 5, 4))

    own[0].wait()
    own[1].wait()
    stage(WKV, 0)
    own[2].wait()
    stage(WQ, 0)

    rows = x_ref.shape[0]

    @pl.loop(0, rows // 64)
    def _(n):
        here = pl.ds(n * 64, 64)
        wide = x_ref[here, :].astype(F32)
        scale = lax.rsqrt(jnp.mean(wide * wide, -1, keepdims=True) + 1e-6)
        a_s[here, :] = (wide * scale * gain_ref[...].astype(F32)).astype(BF16)

    place = (me * rows + lax.broadcasted_iota(jnp.int32, (rows, HEAD // 2), 0)).astype(F32)
    angle = place * freq_ref[...]
    cos_s[...] = jnp.cos(angle)
    sin_s[...] = jnp.sin(angle)

    def turned(t):
        t = t.astype(BF16).astype(F32)
        a, b, cos, sin = t[:, : HEAD // 2], t[:, HEAD // 2 :], cos_s[...], sin_s[...]
        return jnp.concatenate([a * cos - b * sin, b * cos + a * sin], -1)

    for n in range(1, 5):
        stage(WKV, n)
        stage(WQ, n)
    stage(WKV, 5)
    others(WKV)

    kv = dot(a_s[...], wkvb[...].reshape(-1, 2 * HEAD))
    kvb[columns[0], z, core, 0:HEAD, :] = turned(kv[:, :HEAD]).astype(BF16)
    kvb[columns[0], z, core, HEAD:, :] = kv[:, HEAD:].astype(BF16).astype(F32).T.astype(BF16)
    stage(KV, 0)
    stage(WQ, 5)
    others(WQ)

    heads = wqb.shape[4] // HEAD

    @pl.loop(0, heads)
    def _(h):
        cols = pl.ds(pl.multiple_of(h * HEAD, HEAD), HEAD)
        q = dot(a_s[...], wqb[:, :, :, :, cols].reshape(-1, HEAD))
        qt_s[:, cols] = turned(q).T.astype(BF16)

    e = HEAD**-0.5 * LOG2E
    width = qt_s.shape[1]
    strip = 512
    strips = range(0, width, strip)
    keys = 2 * rows
    ones = jnp.ones((8, keys), BF16)

    def step(column, at, masked):
        k = kvb[column, at, :, 0:HEAD, :].reshape(keys, HEAD)
        v = jnp.concatenate([kvb[column, at, 0, HEAD:, :], kvb[column, at, 1, HEAD:, :]], axis=1)
        v = jnp.concatenate([v, ones], axis=0)
        scores = [dot(k, qt_s[:, n : n + strip]) for n in strips]
        weights, keeps = [], []
        for n, s in zip(strips, scores):
            if masked:
                ahead = lax.rem(lax.broadcasted_iota(jnp.int32, s.shape, 1), rows) - lax.broadcasted_iota(jnp.int32, s.shape, 0)
                s = jnp.where(ahead >= -rows * core, s, HIDDEN)
                top = s.max(axis=0, keepdims=True)
            else:
                old = top_s[0:1, n : n + strip]
                top = jnp.maximum(old, s.max(axis=0, keepdims=True))
                keeps.append(jnp.exp2((old - top) * e))
            top_s[0:1, n : n + strip] = top
            weights.append(jnp.exp2((s - top) * e).astype(BF16))
        for i, n in enumerate(strips):
            add = dot(v, weights[i])
            mix_s[:, n : n + strip] = add if masked else mix_s[:, n : n + strip] * keeps[i] + add

    stage(KV, 1)
    stage(KV, 2)
    other(KV, 0, 0)
    step(columns[0], z, True)

    @pl.loop(1, 16)
    def _(i):
        def at(n, *todo):
            @pl.when(i == n)
            def _():
                for do in todo:
                    do()

        for r in range(4):
            for q in range(4):
                n = 4 * r + q
                todo = []
                for u, m in WORK.get(n, ()):
                    if (u, m) == (WO, 0):
                        todo.append(own[3].wait)
                    todo.append(functools.partial(stage, u, m))
                if n:
                    todo.append(functools.partial(other, KV, r, q))
                    at(n, *todo)

        r, q = lax.div(i, 4), lax.rem(i, 4)
        rank = jnp.where(r == 0, ranks[0], jnp.where(r == 1, ranks[1], jnp.where(r == 2, ranks[2], ranks[3])))
        column = jnp.where(q == 0, columns[0], jnp.where(q == 1, columns[1], jnp.where(q == 2, columns[2], columns[3])))

        @pl.when(column * 4 + rank < chip)
        def _():
            step(column, rank, False)

    @pl.loop(0, heads)
    def _(h):
        cols = pl.ds(pl.multiple_of(h * HEAD, HEAD), HEAD)
        o = mix_s[0:HEAD, cols] * (1 / mix_s[HEAD : HEAD + 1, cols])
        seen_s[:, cols] = o.T.astype(BF16)

    stage(WO, 4)
    stage(WO, 5)
    others(WO)

    @pl.loop(0, out_ref.shape[1] // HEAD)
    def _(n):
        cols = pl.ds(pl.multiple_of(n * HEAD, HEAD), HEAD)
        got = dot(seen_s[...], wob[:, :, :, :, cols].reshape(-1, HEAD))
        out_ref[:, cols] = (x_ref[:, cols].astype(F32) + got).astype(BF16)

    for u in range(4):
        copies = [copy for r in range(4) for q in range(4) for copy in sends(u, r, q)]
        if u != WKV:
            copies += [copy for n in range(6) for copy in late_sends(u, n)]
        for copy, when in copies:
            given(when, copy.wait_send)


def solution(mesh):
    half = HEAD // 2
    freq = (float(THETA) ** (-np.arange(half, dtype=np.float64) / half)).astype(np.float32)[None]

    def step(x, gain, wq, wk, wv, wo):
        rows, wide = x.shape
        deep, width = wq.shape
        vmem, hbm = pl.BlockSpec(memory_space=pltpu.VMEM), pl.BlockSpec(memory_space=pltpu.HBM)
        dma = pltpu.SemaphoreType.DMA
        return pl.pallas_call(
            kernel,
            out_shape=jax.ShapeDtypeStruct((rows, wide), BF16),
            in_specs=[vmem] * 3 + [hbm] * 4,
            out_specs=vmem,
            scratch_shapes=[
                pltpu.VMEM((4, 4, 2, deep, width), BF16),
                pltpu.VMEM((4, 4, 2, deep, wide), BF16),
                pltpu.VMEM((4, 4, 2, deep, 2 * HEAD), BF16),
                pltpu.VMEM((4, 4, 2, 2 * HEAD, HEAD), BF16),
                pltpu.VMEM((rows, wide), BF16),
                pltpu.VMEM((HEAD, width), BF16),
                pltpu.VMEM((HEAD + 8, width), F32),
                pltpu.VMEM((8, width), F32),
                pltpu.VMEM((rows, width), BF16),
                pltpu.VMEM((rows, half), F32),
                pltpu.VMEM((rows, half), F32),
                dma((4,)),
                *[dma((4, 4))] * 11,
                *[dma((4, 16))] * 2,
                *[dma((4, 4))] * 7,
            ],
            compiler_params=pltpu.CompilerParams(collective_id=0, has_side_effects=True, vmem_limit_bytes=63 * 2**20),
        )(x, gain[None], jnp.asarray(freq), wq, wk, wv, wo)

    tokens, whole = P(("dp", "sp"), None), P("sp", None)
    return jax.shard_map(step, mesh=mesh, in_specs=(tokens, P(None), whole, whole, whole, whole), out_specs=tokens, check_vma=False)
```

```python
import functools

import jax
import jax.numpy as jnp
import numpy as np
from jax import lax
from jax.experimental import pallas as pl
from jax.experimental.pallas import tpu as pltpu
from jax.sharding import PartitionSpec as P

HEAD = 256
THETA = 10000
LOG2E = 1.4426950408889634
HIDDEN = -1e30
MESH = pl.DeviceIdType.MESH
F32, BF16 = jnp.float32, jnp.bfloat16
WKV, WQ, KV, WO = range(4)

STAGES = (
    ((0, 0),),
    ((1, 0), (0, 1), (0, 2)),
    ((2, 0), (1, 1), (1, 2), (0, 3)),
    ((3, 0), (2, 1), (2, 2), (1, 3)),
    ((3, 1), (3, 2), (2, 3)),
    ((3, 3),),
)
MAIN, A, B, LATE, LATE_A, LATE_B = range(6)
CUTS = {
    WKV: (1, ((0, 512), (0, 256), (256, 256), None, None, None)),
    WQ: (1, ((0, 1536), (0, 768), (768, 768), (1536, 512), (1536, 256), (1792, 256))),
    KV: (0, ((0, 384), (0, 192), (192, 192), (384, 128), (384, 64), (448, 64))),
    WO: (1, ((0, 1536), (0, 768), (768, 768), (1536, 512), (1536, 256), (1792, 256))),
}


WORK = {3: ((KV, 3),), 4: ((WO, 2),), 7: ((KV, 4),), 8: ((WO, 3),), 11: ((KV, 5),), 12: ((WO, 4),), 15: ((WO, 5),)}


def dot(a, b):
    return jnp.dot(a, b, preferred_element_type=F32)


def kernel(x_hbm, gain_ref, freq_ref, wq_ref, wk_ref, wv_ref, wo_ref, out_hbm,
           wqb, wob, wkvb, kvb, x_ref, out_ref, a_s, qt_s, mix_s, acc_s, top_s, cos_s, sin_s,
           local_sem, out_sem, up_s, down_s, z_r, x_s, x_r, y_s, y_r, ha_s, ha_r, hb_s, hb_r, p_s, p_r,
           late_s, late_r, late_up_s, late_down_s, late_z_r, late_p_s, late_p_r):
    me = lax.axis_index("sp")
    core, chip = lax.rem(me, 2), lax.div(me, 2)
    z, y, x = lax.rem(chip, 4), lax.rem(lax.div(chip, 4), 2), lax.div(chip, 8)
    ranks = (z, z + 1 - 2 * lax.rem(z, 2), jnp.where(z >= 2, 1, 2), jnp.where(z >= 2, 0, 3))
    columns = (x * 2 + y, x * 2 + 1 - y, (1 - x) * 2 + y, (1 - x) * 2 + 1 - y)
    above, below, partner = me + 2, me - 2, me + 1 - 2 * core
    x_peer, y_peer = columns[2] * 8 + z * 2 + core, columns[1] * 8 + z * 2 + core
    bufs = (wkvb, wqb, kvb, wob)

    def remote(src, send_sem, recv_sem, to):
        return pltpu.make_async_remote_copy(src_ref=src, dst_ref=src, send_sem=send_sem, recv_sem=recv_sem, device_id={"sp": to}, device_id_type=MESH)

    def given(when, do):
        if when is None:
            do()
        else:
            pl.when(when)(do)

    def arrived(ref, recv_sem):
        pltpu.make_async_remote_copy(src_ref=ref, dst_ref=ref, send_sem=recv_sem, recv_sem=recv_sem, device_id={"sp": partner}, device_id_type=MESH).wait_recv()

    def piece(u, r, q, c, which):
        axis, cuts = CUTS[u]
        start, size = cuts[which]
        column = slice(None) if q is None else columns[q]
        here = pl.ds(start, size)
        return bufs[u].at[column, ranks[r], c, here] if axis == 0 else bufs[u].at[column, ranks[r], c, :, here]

    def sends(u, r, q):
        ref = piece(u, r, q, core, MAIN)
        copies = [(remote(ref, p_s.at[u, 4 * q + r], p_r.at[u, 4 * q + r], partner), None)]
        if q == 0:
            at = ranks[r]
            copies = [
                (remote(ref, up_s.at[u, r], z_r.at[u, at], above), (at <= z) & (z < 3)),
                (remote(ref, down_s.at[u, r], z_r.at[u, at], below), (at >= z) & (z > 0)),
                (remote(ref, x_s.at[u, r], x_r.at[u, r], x_peer), None),
                (remote(ref, y_s.at[u, r], y_r.at[u, r], y_peer), None),
            ] + copies
        elif q == 1:
            copies = [(remote(piece(u, r, q, core, B), hb_s.at[u, r], hb_r.at[u, r], x_peer), None)] + copies
        elif q == 2:
            copies = [(remote(piece(u, r, q, core, A), ha_s.at[u, r], ha_r.at[u, r], y_peer), None)] + copies
        return copies

    def event(u, r, q):
        if q == 0 and r:
            arrived(piece(u, r, q, core, MAIN), z_r.at[u, ranks[r]])
        elif q == 1:
            arrived(piece(u, r, q, core, MAIN), y_r.at[u, r])
        elif q == 2:
            arrived(piece(u, r, q, core, MAIN), x_r.at[u, r])
        elif q == 3:
            arrived(piece(u, r, q, core, A), ha_r.at[u, r])
            arrived(piece(u, r, q, core, B), hb_r.at[u, r])
        for copy, when in sends(u, r, q):
            given(when, copy.start)

    def late_sends(u, n):
        if n == 0:
            ref = piece(u, 0, 0, core, LATE)
            return [(remote(ref, late_s.at[u, 0], late_r.at[u, 0], x_peer), None), (remote(ref, late_s.at[u, 1], late_r.at[u, 1], y_peer), None)]
        if n == 1:
            return [
                (remote(piece(u, 0, 2, core, LATE_A), late_s.at[u, 2], late_r.at[u, 2], y_peer), None),
                (remote(piece(u, 0, 1, core, LATE_B), late_s.at[u, 3], late_r.at[u, 3], x_peer), None),
            ]
        r = n - 2
        at, ref = ranks[r], piece(u, r, None, core, LATE)
        return [
            (remote(ref, late_up_s.at[u, r], late_z_r.at[u, at], above), (at <= z) & (z < 3)),
            (remote(ref, late_down_s.at[u, r], late_z_r.at[u, at], below), (at >= z) & (z > 0)),
            (remote(ref, late_p_s.at[u, r], late_p_r.at[u, r], partner), None),
        ]

    def late_event(u, n):
        if n == 1:
            arrived(piece(u, 0, 2, core, LATE), late_r.at[u, 0])
            arrived(piece(u, 0, 1, core, LATE), late_r.at[u, 1])
        elif n == 2:
            arrived(piece(u, 0, 3, core, LATE_A), late_r.at[u, 2])
            arrived(piece(u, 0, 3, core, LATE_B), late_r.at[u, 3])
        elif n > 2:
            arrived(piece(u, n - 2, None, core, LATE), late_z_r.at[u, ranks[n - 2]])
        for copy, when in late_sends(u, n):
            given(when, copy.start)

    def stage(u, n):
        if u != WKV:
            late_event(u, n)
        for r, q in STAGES[n]:
            event(u, r, q)

    def other(u, r, q):
        arrived(piece(u, r, q, 1 - core, MAIN), p_r.at[u, 4 * q + r])
        if u != WKV and q == 0:
            arrived(piece(u, r, None, 1 - core, LATE), late_p_r.at[u, r])

    def others(u):
        for r in range(4):
            for q in range(4):
                other(u, r, q)

    own = [
        pltpu.make_async_copy(wk_ref, wkvb.at[columns[0], z, core, :, pl.ds(0, HEAD)], local_sem.at[0]),
        pltpu.make_async_copy(wv_ref, wkvb.at[columns[0], z, core, :, pl.ds(HEAD, HEAD)], local_sem.at[1]),
        pltpu.make_async_copy(wq_ref, wqb.at[columns[0], z, core], local_sem.at[2]),
        pltpu.make_async_copy(wo_ref, wob.at[columns[0], z, core], local_sem.at[3]),
        pltpu.make_async_copy(x_hbm, x_ref, local_sem.at[4]),
    ]
    for copy in own:
        copy.start()

    barrier = pltpu.get_barrier_semaphore()

    def greet(to):
        pl.semaphore_signal(barrier, inc=1, device_id={"sp": to}, device_id_type=MESH)

    for to in (x_peer, y_peer, partner):
        greet(to)
    pl.when(z < 3)(lambda: greet(above))
    pl.when(z > 0)(lambda: greet(below))
    pl.semaphore_wait(barrier, jnp.where((z > 0) & (z < 3), 5, 4))

    own[0].wait()
    own[1].wait()
    stage(WKV, 0)
    own[2].wait()
    stage(WQ, 0)

    rows = x_ref.shape[0]

    own[4].wait()
    gain = gain_ref[...].astype(F32).reshape(1, -1)

    @pl.loop(0, rows // 64)
    def _(n):
        here = pl.ds(n * 64, 64)
        wide = x_ref[here, :].astype(F32)
        scale = lax.rsqrt(jnp.mean(wide * wide, -1, keepdims=True) + 1e-6)
        a = (wide * scale * gain).astype(BF16)
        for i in range(16):
            a_s[i // 4, i % 4, here, :] = a[:, i * 128 : (i + 1) * 128]

    place = (me * rows + lax.broadcasted_iota(jnp.int32, (rows, HEAD // 2), 0)).astype(F32)
    angle = place * freq_ref[...]
    cos_s[...] = jnp.cos(angle)
    sin_s[...] = jnp.sin(angle)

    def turned(t):
        t = t.astype(BF16).astype(F32)
        a, b, cos, sin = t[:, : HEAD // 2], t[:, HEAD // 2 :], cos_s[...], sin_s[...]
        return jnp.concatenate([a * cos - b * sin, b * cos + a * sin], -1)

    wide = wqb.shape[4]

    def strip_of(ref, ranks_in):
        return jnp.concatenate([ref[q, r] for r in ranks_in for q in range(4)], axis=1)

    def partial(ref, weights, ranks_in, into, first):
        left = strip_of(ref, ranks_in)

        @pl.loop(0, wide // 512)
        def _(n):
            cols = pl.ds(pl.multiple_of(n * 512, 512), 512)
            right = jnp.concatenate([weights[:, r, :, :, cols].reshape(-1, 512) for r in ranks_in], axis=0)
            got = dot(left, right)
            into[0:rows, cols] = got if first else into[0:rows, cols] + got

    def rank_in(u, r):
        for q in range(4):
            other(u, r, q)

    for n in range(1, 5):
        stage(WKV, n)
        stage(WQ, n)
        if n == 3:
            own[3].wait()
            stage(WO, 0)
        if n >= 2:
            rank_in(WQ, n - 2)
            partial(a_s, wqb, [ranks[n - 2]], mix_s, n == 2)
    stage(WKV, 5)
    others(WKV)

    kv = dot(strip_of(a_s, range(4)), jnp.concatenate([wkvb[:, r].reshape(-1, 2 * HEAD) for r in range(4)], axis=0))
    kvb[columns[0], z, core, 0:HEAD, :] = turned(kv[:, :HEAD]).astype(BF16)
    kvb[columns[0], z, core, HEAD:, :] = kv[:, HEAD:].astype(BF16).astype(F32).T.astype(BF16)
    stage(KV, 0)
    stage(WQ, 5)
    stage(WO, 1)
    rank_in(WQ, 3)
    partial(a_s, wqb, [ranks[3]], mix_s, False)

    heads = wide // HEAD

    @pl.loop(0, heads)
    def _(h):
        cols = pl.ds(pl.multiple_of(h * HEAD, HEAD), HEAD)
        qt_s[:, cols] = turned(mix_s[0:rows, cols]).T.astype(BF16)

    e = HEAD**-0.5 * LOG2E
    width = qt_s.shape[1]
    strip = 512
    strips = range(0, width, strip)
    keys = 2 * rows
    ones = jnp.ones((8, keys), BF16)

    def step(column, at, masked):
        k = kvb[column, at, :, 0:HEAD, :].reshape(keys, HEAD)
        v = jnp.concatenate([kvb[column, at, 0, HEAD:, :], kvb[column, at, 1, HEAD:, :]], axis=1)
        v = jnp.concatenate([v, ones], axis=0)
        scores = [dot(k, qt_s[:, n : n + strip]) for n in strips]
        weights, keeps = [], []
        for n, s in zip(strips, scores):
            if masked:
                ahead = lax.rem(lax.broadcasted_iota(jnp.int32, s.shape, 1), rows) - lax.broadcasted_iota(jnp.int32, s.shape, 0)
                s = jnp.where(ahead >= -rows * core, s, HIDDEN)
                top = s.max(axis=0, keepdims=True)
            else:
                old = top_s[0:1, n : n + strip]
                top = jnp.maximum(old, s.max(axis=0, keepdims=True))
                keeps.append(jnp.exp2((old - top) * e))
            top_s[0:1, n : n + strip] = top
            weights.append(jnp.exp2((s - top) * e).astype(BF16))
        for i, n in enumerate(strips):
            add = dot(v, weights[i])
            mix_s[:, n : n + strip] = add if masked else mix_s[:, n : n + strip] * keeps[i] + add

    stage(KV, 1)
    stage(KV, 2)
    other(KV, 0, 0)
    step(columns[0], z, True)

    @pl.loop(1, 16)
    def _(i):
        def at(n, *todo):
            @pl.when(i == n)
            def _():
                for do in todo:
                    do()

        for r in range(4):
            for q in range(4):
                n = 4 * r + q
                todo = []
                for u, m in WORK.get(n, ()):
                    todo.append(functools.partial(stage, u, m))
                if n:
                    todo.append(functools.partial(other, KV, r, q))
                    at(n, *todo)

        r, q = lax.div(i, 4), lax.rem(i, 4)
        rank = jnp.where(r == 0, ranks[0], jnp.where(r == 1, ranks[1], jnp.where(r == 2, ranks[2], ranks[3])))
        column = jnp.where(q == 0, columns[0], jnp.where(q == 1, columns[1], jnp.where(q == 2, columns[2], columns[3])))

        @pl.when(column * 4 + rank < chip)
        def _():
            step(column, rank, False)

    @pl.loop(0, heads)
    def _(h):
        cols = pl.ds(pl.multiple_of(h * HEAD, HEAD), HEAD)
        o = (mix_s[0:HEAD, cols] * (1 / mix_s[HEAD : HEAD + 1, cols])).T.astype(BF16)
        column, at = lax.div(h, 2), 2 * lax.rem(h, 2)
        a_s[column, at] = o[:, : HEAD // 2]
        a_s[column, at + 1] = o[:, HEAD // 2 :]

    for r in range(3):
        rank_in(WO, r)
    partial(a_s, wob, ranks[:3], acc_s, True)
    rank_in(WO, 3)
    left = strip_of(a_s, ranks[3:])
    stores = []
    for n in range(0, out_ref.shape[1], 512):
        cols = pl.ds(n, 512)
        got = acc_s[:, cols] + dot(left, wob[:, ranks[3], :, :, cols].reshape(-1, 512))
        out_ref[:, cols] = (x_ref[:, cols].astype(F32) + got).astype(BF16)
        stores.append(pltpu.make_async_copy(out_ref.at[:, cols], out_hbm.at[:, cols], out_sem.at[n // 512]))
        stores[-1].start()
    for copy in stores:
        copy.wait()

    for u in range(4):
        copies = [copy for r in range(4) for q in range(4) for copy in sends(u, r, q)]
        if u != WKV:
            copies += [copy for n in range(6) for copy in late_sends(u, n)]
        for copy, when in copies:
            given(when, copy.wait_send)


def solution(mesh):
    half = HEAD // 2
    freq = (float(THETA) ** (-np.arange(half, dtype=np.float64) / half)).astype(np.float32)[None]

    def step(x, gain, wq, wk, wv, wo):
        rows, wide = x.shape
        deep, width = wq.shape
        vmem, hbm = pl.BlockSpec(memory_space=pltpu.VMEM), pl.BlockSpec(memory_space=pltpu.HBM)
        dma = pltpu.SemaphoreType.DMA
        return pl.pallas_call(
            kernel,
            out_shape=jax.ShapeDtypeStruct((rows, wide), BF16),
            in_specs=[hbm, vmem, vmem] + [hbm] * 4,
            out_specs=hbm,
            scratch_shapes=[
                pltpu.VMEM((4, 4, 2, deep, width), BF16),
                pltpu.VMEM((4, 4, 2, deep, wide), BF16),
                pltpu.VMEM((4, 4, 2, deep, 2 * HEAD), BF16),
                pltpu.VMEM((4, 4, 2, 2 * HEAD, HEAD), BF16),
                pltpu.VMEM((rows, wide), BF16),
                pltpu.VMEM((rows, wide), BF16),
                pltpu.VMEM((4, 4, rows, 2 * deep), BF16),
                pltpu.VMEM((HEAD, width), BF16),
                pltpu.VMEM((HEAD + 8, width), F32),
                pltpu.VMEM((rows, wide), F32),
                pltpu.VMEM((8, width), F32),
                pltpu.VMEM((rows, half), F32),
                pltpu.VMEM((rows, half), F32),
                dma((5,)),
                dma((4,)),
                *[dma((4, 4))] * 11,
                *[dma((4, 16))] * 2,
                *[dma((4, 4))] * 7,
            ],
            compiler_params=pltpu.CompilerParams(collective_id=0, has_side_effects=True, vmem_limit_bytes=63 * 2**20),
        )(x, gain, jnp.asarray(freq), wq, wk, wv, wo)

    tokens, whole = P(("dp", "sp"), None), P("sp", None)
    return jax.shard_map(step, mesh=mesh, in_specs=(tokens, P(None), whole, whole, whole, whole), out_specs=tokens, check_vma=False)
```

```python
import functools

import jax
import jax.numpy as jnp
import numpy as np
from jax import lax
from jax.experimental import pallas as pl
from jax.experimental.pallas import tpu as pltpu
from jax.sharding import PartitionSpec as P

HEAD = 256
THETA = 10000
LOG2E = 1.4426950408889634
HIDDEN = -1e30
MESH = pl.DeviceIdType.MESH
F32, BF16 = jnp.float32, jnp.bfloat16
WKV, WQ, KV, WO = range(4)

STAGES = (
    ((0, 0),),
    ((1, 0), (0, 1), (0, 2)),
    ((2, 0), (1, 1), (1, 2), (0, 3)),
    ((3, 0), (2, 1), (2, 2), (1, 3)),
    ((3, 1), (3, 2), (2, 3)),
    ((3, 3),),
)
MAIN, A, B, LATE, LATE_A, LATE_B = range(6)
CUTS = {
    WKV: (1, ((0, 512), (0, 256), (256, 256), None, None, None)),
    WQ: (1, ((0, 1536), (0, 768), (768, 768), (1536, 512), (1536, 256), (1792, 256))),
    KV: (0, ((0, 400), (0, 192), (192, 208), (400, 112), (400, 64), (464, 48))),
    WO: (1, ((0, 1664), (0, 768), (768, 896), (1664, 384), (1664, 256), (1920, 128))),
}


WORK = {1: ((KV, 3),), 3: ((WO, 2),), 7: ((KV, 4),), 10: ((WO, 3),), 11: ((KV, 5),), 14: ((WO, 4),)}


def dot(a, b):
    return jnp.dot(a, b, preferred_element_type=F32)


def kernel(x_hbm, gain_ref, freq_ref, wq_ref, wk_ref, wv_ref, wo_ref, out_hbm,
           wqb, wob, wkvb, kvb, x_ref, out_ref, a_s, qt_s, mix_s, acc_s, top_s, cos_s, sin_s,
           local_sem, out_sem, up_s, down_s, z_r, x_s, x_r, y_s, y_r, ha_s, ha_r, hb_s, hb_r, p_s, p_r,
           late_s, late_r, late_up_s, late_down_s, late_z_r, late_p_s, late_p_r):
    me = lax.axis_index("sp")
    core, chip = lax.rem(me, 2), lax.div(me, 2)
    z, y, x = lax.rem(chip, 4), lax.rem(lax.div(chip, 4), 2), lax.div(chip, 8)
    ranks = (z, z + 1 - 2 * lax.rem(z, 2), jnp.where(z >= 2, 1, 2), jnp.where(z >= 2, 0, 3))
    columns = (x * 2 + y, x * 2 + 1 - y, (1 - x) * 2 + y, (1 - x) * 2 + 1 - y)
    above, below, partner = me + 2, me - 2, me + 1 - 2 * core
    x_peer, y_peer = columns[2] * 8 + z * 2 + core, columns[1] * 8 + z * 2 + core
    bufs = (wkvb, wqb, kvb, wob)

    def remote(src, send_sem, recv_sem, to):
        return pltpu.make_async_remote_copy(src_ref=src, dst_ref=src, send_sem=send_sem, recv_sem=recv_sem, device_id={"sp": to}, device_id_type=MESH)

    def given(when, do):
        if when is None:
            do()
        else:
            pl.when(when)(do)

    def arrived(ref, recv_sem):
        pltpu.make_async_remote_copy(src_ref=ref, dst_ref=ref, send_sem=recv_sem, recv_sem=recv_sem, device_id={"sp": partner}, device_id_type=MESH).wait_recv()

    def piece(u, r, q, c, which):
        axis, cuts = CUTS[u]
        start, size = cuts[which]
        column = slice(None) if q is None else columns[q]
        here = pl.ds(start, size)
        return bufs[u].at[column, ranks[r], c, here] if axis == 0 else bufs[u].at[column, ranks[r], c, :, here]

    def sends(u, r, q):
        ref = piece(u, r, q, core, MAIN)
        copies = [(remote(ref, p_s.at[u, 4 * q + r], p_r.at[u, 4 * q + r], partner), None)]
        if q == 0:
            at = ranks[r]
            copies = [
                (remote(ref, up_s.at[u, r], z_r.at[u, at], above), (at <= z) & (z < 3)),
                (remote(ref, down_s.at[u, r], z_r.at[u, at], below), (at >= z) & (z > 0)),
                (remote(ref, x_s.at[u, r], x_r.at[u, r], x_peer), None),
                (remote(ref, y_s.at[u, r], y_r.at[u, r], y_peer), None),
            ] + copies
        elif q == 1:
            copies = [(remote(piece(u, r, q, core, B), hb_s.at[u, r], hb_r.at[u, r], x_peer), None)] + copies
        elif q == 2:
            copies = [(remote(piece(u, r, q, core, A), ha_s.at[u, r], ha_r.at[u, r], y_peer), None)] + copies
        return copies

    def event(u, r, q):
        if q == 0 and r:
            arrived(piece(u, r, q, core, MAIN), z_r.at[u, ranks[r]])
        elif q == 1:
            arrived(piece(u, r, q, core, MAIN), y_r.at[u, r])
        elif q == 2:
            arrived(piece(u, r, q, core, MAIN), x_r.at[u, r])
        elif q == 3:
            arrived(piece(u, r, q, core, A), ha_r.at[u, r])
            arrived(piece(u, r, q, core, B), hb_r.at[u, r])
        for copy, when in sends(u, r, q):
            given(when, copy.start)

    def late_sends(u, n):
        if n == 0:
            ref = piece(u, 0, 0, core, LATE)
            return [(remote(ref, late_s.at[u, 0], late_r.at[u, 0], x_peer), None), (remote(ref, late_s.at[u, 1], late_r.at[u, 1], y_peer), None)]
        if n == 1:
            return [
                (remote(piece(u, 0, 2, core, LATE_A), late_s.at[u, 2], late_r.at[u, 2], y_peer), None),
                (remote(piece(u, 0, 1, core, LATE_B), late_s.at[u, 3], late_r.at[u, 3], x_peer), None),
            ]
        r = n - 2
        at, ref = ranks[r], piece(u, r, None, core, LATE)
        return [
            (remote(ref, late_up_s.at[u, r], late_z_r.at[u, at], above), (at <= z) & (z < 3)),
            (remote(ref, late_down_s.at[u, r], late_z_r.at[u, at], below), (at >= z) & (z > 0)),
            (remote(ref, late_p_s.at[u, r], late_p_r.at[u, r], partner), None),
        ]

    def late_event(u, n):
        if n == 1:
            arrived(piece(u, 0, 2, core, LATE), late_r.at[u, 0])
            arrived(piece(u, 0, 1, core, LATE), late_r.at[u, 1])
        elif n == 2:
            arrived(piece(u, 0, 3, core, LATE_A), late_r.at[u, 2])
            arrived(piece(u, 0, 3, core, LATE_B), late_r.at[u, 3])
        elif n > 2:
            arrived(piece(u, n - 2, None, core, LATE), late_z_r.at[u, ranks[n - 2]])
        for copy, when in late_sends(u, n):
            given(when, copy.start)

    def stage(u, n):
        if u != WKV:
            late_event(u, n)
        for r, q in STAGES[n]:
            event(u, r, q)

    def other(u, r, q):
        arrived(piece(u, r, q, 1 - core, MAIN), p_r.at[u, 4 * q + r])
        if u != WKV and q == 0:
            arrived(piece(u, r, None, 1 - core, LATE), late_p_r.at[u, r])

    def others(u):
        for r in range(4):
            for q in range(4):
                other(u, r, q)

    own = [
        pltpu.make_async_copy(wk_ref, wkvb.at[columns[0], z, core, :, pl.ds(0, HEAD)], local_sem.at[0]),
        pltpu.make_async_copy(wv_ref, wkvb.at[columns[0], z, core, :, pl.ds(HEAD, HEAD)], local_sem.at[1]),
        pltpu.make_async_copy(wq_ref, wqb.at[columns[0], z, core], local_sem.at[2]),
        pltpu.make_async_copy(wo_ref, wob.at[columns[0], z, core], local_sem.at[3]),
        pltpu.make_async_copy(x_hbm, x_ref, local_sem.at[4]),
    ]
    for copy in own:
        copy.start()

    barrier = pltpu.get_barrier_semaphore()

    def greet(to):
        pl.semaphore_signal(barrier, inc=1, device_id={"sp": to}, device_id_type=MESH)

    for to in (x_peer, y_peer, partner):
        greet(to)
    pl.when(z < 3)(lambda: greet(above))
    pl.when(z > 0)(lambda: greet(below))
    pl.semaphore_wait(barrier, jnp.where((z > 0) & (z < 3), 5, 4))

    own[0].wait()
    own[1].wait()
    stage(WKV, 0)
    own[2].wait()
    stage(WQ, 0)

    rows = x_ref.shape[0]

    own[4].wait()
    gain = gain_ref[...].astype(F32).reshape(1, -1)

    @pl.loop(0, rows // 64)
    def _(n):
        here = pl.ds(n * 64, 64)
        wide = x_ref[here, :].astype(F32)
        scale = lax.rsqrt(jnp.mean(wide * wide, -1, keepdims=True) + 1e-6)
        a = (wide * scale * gain).astype(BF16)
        for i in range(16):
            a_s[i // 4, i % 4, here, :] = a[:, i * 128 : (i + 1) * 128]

    place = (me * rows + lax.broadcasted_iota(jnp.int32, (rows, HEAD // 2), 0)).astype(F32)
    angle = place * freq_ref[...]
    cos_s[...] = jnp.cos(angle)
    sin_s[...] = jnp.sin(angle)

    def turned(t):
        t = t.astype(BF16).astype(F32)
        a, b, cos, sin = t[:, : HEAD // 2], t[:, HEAD // 2 :], cos_s[...], sin_s[...]
        return jnp.concatenate([a * cos - b * sin, b * cos + a * sin], -1)

    wide = wqb.shape[4]

    def strip_of(ref, ranks_in):
        return jnp.concatenate([ref[q, r] for r in ranks_in for q in range(4)], axis=1)

    def partial(ref, weights, ranks_in, into, first):
        left = strip_of(ref, ranks_in)

        @pl.loop(0, wide // 512)
        def _(n):
            cols = pl.ds(pl.multiple_of(n * 512, 512), 512)
            right = jnp.concatenate([weights[:, r, :, :, cols].reshape(-1, 512) for r in ranks_in], axis=0)
            got = dot(left, right)
            into[0:rows, cols] = got if first else into[0:rows, cols] + got

    def rank_in(u, r):
        for q in range(4):
            other(u, r, q)

    def query(n, first=False):
        rank_in(WQ, n)
        partial(a_s, wqb, [ranks[n]], mix_s, first)

    for u, n in ((WKV, 1), (WKV, 2), (WKV, 3), (WQ, 1)):
        stage(u, n)
    own[3].wait()
    for u, n in ((WO, 0), (WKV, 4), (WQ, 2), (WKV, 5)):
        stage(u, n)
    others(WKV)
    kv = dot(strip_of(a_s, range(4)), jnp.concatenate([wkvb[:, r].reshape(-1, 2 * HEAD) for r in range(4)], axis=0))
    kvb[columns[0], z, core, 0:HEAD, :] = turned(kv[:, :HEAD]).astype(BF16)
    kvb[columns[0], z, core, HEAD:, :] = kv[:, HEAD:].astype(BF16).astype(F32).T.astype(BF16)
    stage(KV, 0)
    query(0, True)
    for u, n in ((WQ, 3), (KV, 1), (WQ, 4), (KV, 2), (WO, 1)):
        stage(u, n)
    query(1)
    stage(WQ, 5)
    query(2)
    query(3)

    heads = wide // HEAD

    @pl.loop(0, heads)
    def _(h):
        cols = pl.ds(pl.multiple_of(h * HEAD, HEAD), HEAD)
        qt_s[:, cols] = turned(mix_s[0:rows, cols]).T.astype(BF16)

    e = HEAD**-0.5 * LOG2E
    width = qt_s.shape[1]
    strip = 512
    strips = range(0, width, strip)
    keys = 2 * rows
    ones = jnp.ones((8, keys), BF16)

    def step(column, at, masked):
        k = kvb[column, at, :, 0:HEAD, :].reshape(keys, HEAD)
        v = jnp.concatenate([kvb[column, at, 0, HEAD:, :], kvb[column, at, 1, HEAD:, :]], axis=1)
        v = jnp.concatenate([v, ones], axis=0)
        scores = [dot(k, qt_s[:, n : n + strip]) for n in strips]
        weights, keeps = [], []
        for n, s in zip(strips, scores):
            if masked:
                ahead = lax.rem(lax.broadcasted_iota(jnp.int32, s.shape, 1), rows) - lax.broadcasted_iota(jnp.int32, s.shape, 0)
                s = jnp.where(ahead >= -rows * core, s, HIDDEN)
                top = s.max(axis=0, keepdims=True)
            else:
                old = top_s[0:1, n : n + strip]
                top = jnp.maximum(old, s.max(axis=0, keepdims=True))
                keeps.append(jnp.exp2((old - top) * e))
            top_s[0:1, n : n + strip] = top
            weights.append(jnp.exp2((s - top) * e).astype(BF16))
        for i, n in enumerate(strips):
            add = dot(v, weights[i])
            mix_s[:, n : n + strip] = add if masked else mix_s[:, n : n + strip] * keeps[i] + add

    other(KV, 0, 0)
    step(columns[0], z, True)

    @pl.loop(1, 16)
    def _(i):
        def at(n, *todo):
            @pl.when(i == n)
            def _():
                for do in todo:
                    do()

        for r in range(4):
            for q in range(4):
                n = 4 * r + q
                todo = []
                for u, m in WORK.get(n, ()):
                    todo.append(functools.partial(stage, u, m))
                if n:
                    todo.append(functools.partial(other, KV, r, q))
                    at(n, *todo)

        r, q = lax.div(i, 4), lax.rem(i, 4)
        rank = jnp.where(r == 0, ranks[0], jnp.where(r == 1, ranks[1], jnp.where(r == 2, ranks[2], ranks[3])))
        column = jnp.where(q == 0, columns[0], jnp.where(q == 1, columns[1], jnp.where(q == 2, columns[2], columns[3])))

        @pl.when(column * 4 + rank < chip)
        def _():
            step(column, rank, False)

    @pl.loop(0, heads)
    def _(h):
        cols = pl.ds(pl.multiple_of(h * HEAD, HEAD), HEAD)
        o = (mix_s[0:HEAD, cols] * (1 / mix_s[HEAD : HEAD + 1, cols])).T.astype(BF16)
        column, at = lax.div(h, 2), 2 * lax.rem(h, 2)
        a_s[column, at] = o[:, : HEAD // 2]
        a_s[column, at + 1] = o[:, HEAD // 2 :]

    stage(WO, 5)
    for r in range(3):
        rank_in(WO, r)
    partial(a_s, wob, ranks[:3], acc_s, True)
    rank_in(WO, 3)
    left = strip_of(a_s, ranks[3:])
    stores = []
    for n in range(0, out_ref.shape[1], 512):
        cols = pl.ds(n, 512)
        got = acc_s[:, cols] + dot(left, wob[:, ranks[3], :, :, cols].reshape(-1, 512))
        out_ref[:, cols] = (x_ref[:, cols].astype(F32) + got).astype(BF16)
        stores.append(pltpu.make_async_copy(out_ref.at[:, cols], out_hbm.at[:, cols], out_sem.at[n // 512]))
        stores[-1].start()
    for copy in stores:
        copy.wait()

    for u in range(4):
        copies = [copy for r in range(4) for q in range(4) for copy in sends(u, r, q)]
        if u != WKV:
            copies += [copy for n in range(6) for copy in late_sends(u, n)]
        for copy, when in copies:
            given(when, copy.wait_send)


def solution(mesh):
    half = HEAD // 2
    freq = (float(THETA) ** (-np.arange(half, dtype=np.float64) / half)).astype(np.float32)[None]

    def step(x, gain, wq, wk, wv, wo):
        rows, wide = x.shape
        deep, width = wq.shape
        vmem, hbm = pl.BlockSpec(memory_space=pltpu.VMEM), pl.BlockSpec(memory_space=pltpu.HBM)
        dma = pltpu.SemaphoreType.DMA
        return pl.pallas_call(
            kernel,
            out_shape=jax.ShapeDtypeStruct((rows, wide), BF16),
            in_specs=[hbm, vmem, vmem] + [hbm] * 4,
            out_specs=hbm,
            scratch_shapes=[
                pltpu.VMEM((4, 4, 2, deep, width), BF16),
                pltpu.VMEM((4, 4, 2, deep, wide), BF16),
                pltpu.VMEM((4, 4, 2, deep, 2 * HEAD), BF16),
                pltpu.VMEM((4, 4, 2, 2 * HEAD, HEAD), BF16),
                pltpu.VMEM((rows, wide), BF16),
                pltpu.VMEM((rows, wide), BF16),
                pltpu.VMEM((4, 4, rows, 2 * deep), BF16),
                pltpu.VMEM((HEAD, width), BF16),
                pltpu.VMEM((HEAD + 8, width), F32),
                pltpu.VMEM((rows, wide), F32),
                pltpu.VMEM((8, width), F32),
                pltpu.VMEM((rows, half), F32),
                pltpu.VMEM((rows, half), F32),
                dma((5,)),
                dma((4,)),
                *[dma((4, 4))] * 11,
                *[dma((4, 16))] * 2,
                *[dma((4, 4))] * 7,
            ],
            compiler_params=pltpu.CompilerParams(collective_id=0, has_side_effects=True, vmem_limit_bytes=63 * 2**20),
        )(x, gain, jnp.asarray(freq), wq, wk, wv, wo)

    tokens, whole = P(("dp", "sp"), None), P("sp", None)
    return jax.shard_map(step, mesh=mesh, in_specs=(tokens, P(None), whole, whole, whole, whole), out_specs=tokens, check_vma=False)
```

```python
import functools

import jax
import jax.numpy as jnp
import numpy as np
from jax import lax
from jax.experimental import pallas as pl
from jax.experimental.pallas import tpu as pltpu
from jax.sharding import PartitionSpec as P

HEAD = 256
THETA = 10000
LOG2E = 1.4426950408889634
HIDDEN = -1e30
MESH = pl.DeviceIdType.MESH
F32, BF16 = jnp.float32, jnp.bfloat16
WKV, WQ, KV, WO = range(4)

STAGES = (
    ((0, 0),),
    ((1, 0), (0, 1), (0, 2)),
    ((2, 0), (1, 1), (1, 2), (0, 3)),
    ((3, 0), (2, 1), (2, 2), (1, 3)),
    ((3, 1), (3, 2), (2, 3)),
    ((3, 3),),
)
MAIN, A, B, LATE, LATE_A, LATE_B = range(6)
CUTS = {
    WKV: (1, ((0, 512), (0, 256), (256, 256), None, None, None)),
    WQ: (1, ((0, 1408), (0, 640), (640, 768), (1408, 640), (1408, 384), (1792, 256))),
    KV: (0, ((0, 400), (0, 192), (192, 208), (400, 112), (400, 64), (464, 48))),
    WO: (1, ((0, 1792), (0, 896), (896, 896), (1792, 256), (1792, 128), (1920, 128))),
}


WORK = {1: ((KV, 3),), 3: ((WO, 2),), 7: ((KV, 4),), 10: ((WO, 3),), 11: ((KV, 5),), 14: ((WO, 4),)}


def dot(a, b):
    return jnp.dot(a, b, preferred_element_type=F32)


def kernel(x_hbm, gain_ref, freq_ref, wq_ref, wk_ref, wv_ref, wo_ref, out_hbm,
           wqb, wob, wkvb, kvb, x_ref, out_ref, a_s, qt_s, mix_s, acc_s, top_s, cos_s, sin_s,
           local_sem, out_sem, up_s, down_s, z_r, x_s, x_r, y_s, y_r, ha_s, ha_r, hb_s, hb_r, p_s, p_r,
           late_s, late_r, late_up_s, late_down_s, late_z_r, late_p_s, late_p_r):
    me = lax.axis_index("sp")
    core, chip = lax.rem(me, 2), lax.div(me, 2)
    z, y, x = lax.rem(chip, 4), lax.rem(lax.div(chip, 4), 2), lax.div(chip, 8)
    ranks = (z, z + 1 - 2 * lax.rem(z, 2), jnp.where(z >= 2, 1, 2), jnp.where(z >= 2, 0, 3))
    columns = (x * 2 + y, x * 2 + 1 - y, (1 - x) * 2 + y, (1 - x) * 2 + 1 - y)
    above, below, partner = me + 2, me - 2, me + 1 - 2 * core
    x_peer, y_peer = columns[2] * 8 + z * 2 + core, columns[1] * 8 + z * 2 + core
    bufs = (wkvb, wqb, kvb, wob)

    def remote(src, send_sem, recv_sem, to):
        return pltpu.make_async_remote_copy(src_ref=src, dst_ref=src, send_sem=send_sem, recv_sem=recv_sem, device_id={"sp": to}, device_id_type=MESH)

    def given(when, do):
        if when is None:
            do()
        else:
            pl.when(when)(do)

    def arrived(ref, recv_sem):
        pltpu.make_async_remote_copy(src_ref=ref, dst_ref=ref, send_sem=recv_sem, recv_sem=recv_sem, device_id={"sp": partner}, device_id_type=MESH).wait_recv()

    def piece(u, r, q, c, which):
        axis, cuts = CUTS[u]
        start, size = cuts[which]
        column = slice(None) if q is None else columns[q]
        here = pl.ds(start, size)
        return bufs[u].at[column, ranks[r], c, here] if axis == 0 else bufs[u].at[column, ranks[r], c, :, here]

    def sends(u, r, q):
        ref = piece(u, r, q, core, MAIN)
        copies = [(remote(ref, p_s.at[u, 4 * q + r], p_r.at[u, 4 * q + r], partner), None)]
        if q == 0:
            at = ranks[r]
            copies = [
                (remote(ref, up_s.at[u, r], z_r.at[u, at], above), (at <= z) & (z < 3)),
                (remote(ref, down_s.at[u, r], z_r.at[u, at], below), (at >= z) & (z > 0)),
                (remote(ref, x_s.at[u, r], x_r.at[u, r], x_peer), None),
                (remote(ref, y_s.at[u, r], y_r.at[u, r], y_peer), None),
            ] + copies
        elif q == 1:
            copies = [(remote(piece(u, r, q, core, B), hb_s.at[u, r], hb_r.at[u, r], x_peer), None)] + copies
        elif q == 2:
            copies = [(remote(piece(u, r, q, core, A), ha_s.at[u, r], ha_r.at[u, r], y_peer), None)] + copies
        return copies

    def event(u, r, q):
        if q == 0 and r:
            arrived(piece(u, r, q, core, MAIN), z_r.at[u, ranks[r]])
        elif q == 1:
            arrived(piece(u, r, q, core, MAIN), y_r.at[u, r])
        elif q == 2:
            arrived(piece(u, r, q, core, MAIN), x_r.at[u, r])
        elif q == 3:
            arrived(piece(u, r, q, core, A), ha_r.at[u, r])
            arrived(piece(u, r, q, core, B), hb_r.at[u, r])
        for copy, when in sends(u, r, q):
            given(when, copy.start)

    def late_sends(u, n):
        if n == 0:
            ref = piece(u, 0, 0, core, LATE)
            return [(remote(ref, late_s.at[u, 0], late_r.at[u, 0], x_peer), None), (remote(ref, late_s.at[u, 1], late_r.at[u, 1], y_peer), None)]
        if n == 1:
            copies = [(remote(piece(u, 0, 2, core, LATE_A), late_s.at[u, 2], late_r.at[u, 2], y_peer), None)]
            if CUTS[u][1][LATE_B]:
                copies.append((remote(piece(u, 0, 1, core, LATE_B), late_s.at[u, 3], late_r.at[u, 3], x_peer), None))
            return copies
        r = n - 2
        at, ref = ranks[r], piece(u, r, None, core, LATE)
        return [
            (remote(ref, late_up_s.at[u, r], late_z_r.at[u, at], above), (at <= z) & (z < 3)),
            (remote(ref, late_down_s.at[u, r], late_z_r.at[u, at], below), (at >= z) & (z > 0)),
            (remote(ref, late_p_s.at[u, r], late_p_r.at[u, r], partner), None),
        ]

    def late_event(u, n):
        if n == 1:
            arrived(piece(u, 0, 2, core, LATE), late_r.at[u, 0])
            arrived(piece(u, 0, 1, core, LATE), late_r.at[u, 1])
        elif n == 2:
            arrived(piece(u, 0, 3, core, LATE_A), late_r.at[u, 2])
            if CUTS[u][1][LATE_B]:
                arrived(piece(u, 0, 3, core, LATE_B), late_r.at[u, 3])
        elif n > 2:
            arrived(piece(u, n - 2, None, core, LATE), late_z_r.at[u, ranks[n - 2]])
        for copy, when in late_sends(u, n):
            given(when, copy.start)

    def stage(u, n):
        if u != WKV:
            late_event(u, n)
        for r, q in STAGES[n]:
            event(u, r, q)

    def other(u, r, q):
        arrived(piece(u, r, q, 1 - core, MAIN), p_r.at[u, 4 * q + r])
        if u != WKV and q == 0:
            arrived(piece(u, r, None, 1 - core, LATE), late_p_r.at[u, r])

    def others(u):
        for r in range(4):
            for q in range(4):
                other(u, r, q)

    own = [
        pltpu.make_async_copy(wk_ref, wkvb.at[columns[0], z, core, :, pl.ds(0, HEAD)], local_sem.at[0]),
        pltpu.make_async_copy(wv_ref, wkvb.at[columns[0], z, core, :, pl.ds(HEAD, HEAD)], local_sem.at[1]),
        pltpu.make_async_copy(wq_ref, wqb.at[columns[0], z, core], local_sem.at[2]),
        pltpu.make_async_copy(wo_ref, wob.at[columns[0], z, core], local_sem.at[3]),
        pltpu.make_async_copy(x_hbm, x_ref, local_sem.at[4]),
    ]
    for copy in own:
        copy.start()

    barrier = pltpu.get_barrier_semaphore()

    def greet(to):
        pl.semaphore_signal(barrier, inc=1, device_id={"sp": to}, device_id_type=MESH)

    for to in (x_peer, y_peer, partner):
        greet(to)
    pl.when(z < 3)(lambda: greet(above))
    pl.when(z > 0)(lambda: greet(below))
    pl.semaphore_wait(barrier, jnp.where((z > 0) & (z < 3), 5, 4))

    rows, wide = x_ref.shape
    heads = wide // HEAD

    def normalise():
        own[4].wait()
        gain = gain_ref[...].astype(F32).reshape(1, -1)

        @pl.loop(0, rows // 64)
        def _(n):
            here = pl.ds(n * 64, 64)
            wide = x_ref[here, :].astype(F32)
            scale = lax.rsqrt(jnp.mean(wide * wide, -1, keepdims=True) + 1e-6)
            a = (wide * scale * gain).astype(BF16)
            for i in range(16):
                a_s[i // 4, i % 4, here, :] = a[:, i * 128 : (i + 1) * 128]

        place = (me * rows + lax.broadcasted_iota(jnp.int32, (rows, HEAD // 2), 0)).astype(F32)
        angle = place * freq_ref[...]
        cos_s[...] = jnp.cos(angle)
        sin_s[...] = jnp.sin(angle)

    def turned(t):
        t = t.astype(BF16).astype(F32)
        a, b, cos, sin = t[:, : HEAD // 2], t[:, HEAD // 2 :], cos_s[...], sin_s[...]
        return jnp.concatenate([a * cos - b * sin, b * cos + a * sin], -1)

    def strip_of(ref, ranks_in):
        return jnp.concatenate([ref[q, r] for r in ranks_in for q in range(4)], axis=1)

    def partial(ref, weights, ranks_in, into, first):
        left = strip_of(ref, ranks_in)

        @pl.loop(0, wide // 512)
        def _(n):
            cols = pl.ds(pl.multiple_of(n * 512, 512), 512)
            right = jnp.concatenate([weights[:, r, :, :, cols].reshape(-1, 512) for r in ranks_in], axis=0)
            got = dot(left, right)
            into[0:rows, cols] = got if first else into[0:rows, cols] + got

    def rank_in(u, r):
        for q in range(4):
            other(u, r, q)

    def query(n, first=False):
        rank_in(WQ, n)
        partial(a_s, wqb, [ranks[n]], mix_s, first)

    def keys_values():
        others(WKV)
        kv = dot(strip_of(a_s, range(4)), jnp.concatenate([wkvb[:, r].reshape(-1, 2 * HEAD) for r in range(4)], axis=0))
        kvb[columns[0], z, core, 0:HEAD, :] = turned(kv[:, :HEAD]).astype(BF16)
        kvb[columns[0], z, core, HEAD:, :] = kv[:, HEAD:].astype(BF16).astype(F32).T.astype(BF16)

    def queries_turned():
        @pl.loop(0, heads)
        def _(h):
            cols = pl.ds(pl.multiple_of(h * HEAD, HEAD), HEAD)
            qt_s[:, cols] = turned(mix_s[0:rows, cols]).T.astype(BF16)

    own[0].wait()
    own[1].wait()
    stage(WKV, 0)
    own[2].wait()
    stage(WQ, 0)
    normalise()
    for u, n in ((WKV, 1), (WKV, 2), (WKV, 3), (WQ, 1)):
        stage(u, n)
    own[3].wait()
    for u, n in ((WO, 0), (WKV, 4), (WQ, 2), (WKV, 5)):
        stage(u, n)
    keys_values()
    stage(KV, 0)
    query(0, True)
    for u, n in ((WQ, 3), (KV, 1), (WQ, 4), (KV, 2), (WO, 1)):
        stage(u, n)
    query(1)
    stage(WQ, 5)
    query(2)
    query(3)
    queries_turned()

    e = HEAD**-0.5 * LOG2E
    width = qt_s.shape[1]
    strip = 512
    strips = range(0, width, strip)
    keys = 2 * rows
    ones = jnp.ones((8, keys), BF16)

    def step(column, at, masked):
        k = kvb[column, at, :, 0:HEAD, :].reshape(keys, HEAD)
        v = jnp.concatenate([kvb[column, at, 0, HEAD:, :], kvb[column, at, 1, HEAD:, :]], axis=1)
        v = jnp.concatenate([v, ones], axis=0)
        scores = [dot(k, qt_s[:, n : n + strip]) for n in strips]
        weights, keeps = [], []
        for n, s in zip(strips, scores):
            if masked:
                ahead = lax.rem(lax.broadcasted_iota(jnp.int32, s.shape, 1), rows) - lax.broadcasted_iota(jnp.int32, s.shape, 0)
                s = jnp.where(ahead >= -rows * core, s, HIDDEN)
                top = s.max(axis=0, keepdims=True)
            else:
                old = top_s[0:1, n : n + strip]
                top = jnp.maximum(old, s.max(axis=0, keepdims=True))
                keeps.append(jnp.exp2((old - top) * e))
            top_s[0:1, n : n + strip] = top
            weights.append(jnp.exp2((s - top) * e).astype(BF16))
        for i, n in enumerate(strips):
            add = dot(v, weights[i])
            mix_s[:, n : n + strip] = add if masked else mix_s[:, n : n + strip] * keeps[i] + add

    other(KV, 0, 0)
    step(columns[0], z, True)

    @pl.loop(1, 16)
    def _(i):
        def at(n, *todo):
            @pl.when(i == n)
            def _():
                for do in todo:
                    do()

        for r in range(4):
            for q in range(4):
                n = 4 * r + q
                todo = []
                for u, m in WORK.get(n, ()):
                    todo.append(functools.partial(stage, u, m))
                if n:
                    todo.append(functools.partial(other, KV, r, q))
                    at(n, *todo)

        r, q = lax.div(i, 4), lax.rem(i, 4)
        rank = jnp.where(r == 0, ranks[0], jnp.where(r == 1, ranks[1], jnp.where(r == 2, ranks[2], ranks[3])))
        column = jnp.where(q == 0, columns[0], jnp.where(q == 1, columns[1], jnp.where(q == 2, columns[2], columns[3])))

        @pl.when(column * 4 + rank < chip)
        def _():
            step(column, rank, False)

    def attended():
        @pl.loop(0, heads)
        def _(h):
            cols = pl.ds(pl.multiple_of(h * HEAD, HEAD), HEAD)
            o = (mix_s[0:HEAD, cols] * (1 / mix_s[HEAD : HEAD + 1, cols])).T.astype(BF16)
            column, at = lax.div(h, 2), 2 * lax.rem(h, 2)
            a_s[column, at] = o[:, : HEAD // 2]
            a_s[column, at + 1] = o[:, HEAD // 2 :]

    stores = []

    def finish(left, ranks_in, start, first, last):
        for n in range(start, start + 1024, 512):
            cols = pl.ds(n, 512)
            got = dot(left, jnp.concatenate([wob[:, r, :, :, cols].reshape(-1, 512) for r in ranks_in], axis=0))
            if not first:
                got = acc_s[:, cols] + got
            if last:
                out_ref[:, cols] = (x_ref[:, cols].astype(F32) + got).astype(BF16)
            else:
                acc_s[:, cols] = got
        if last:
            cols = pl.ds(start, 1024)
            stores.append(pltpu.make_async_copy(out_ref.at[:, cols], out_hbm.at[:, cols], out_sem.at[len(stores)]))
            stores[-1].start()

    attended()
    stage(WO, 5)
    for r in range(3):
        rank_in(WO, r)
    for at in (0, 1024):
        finish(strip_of(a_s, ranks[:3]), ranks[:3], at, True, False)
    rank_in(WO, 3)
    for at in (0, 1024):
        finish(strip_of(a_s, ranks[3:]), ranks[3:], at, False, True)
    for copy in stores:
        copy.wait()

    for u in CUTS:
        copies = [copy for r in range(4) for q in range(4) for copy in sends(u, r, q)]
        if u != WKV:
            copies += [copy for n in range(6) for copy in late_sends(u, n)]
        for copy, when in copies:
            given(when, copy.wait_send)


def solution(mesh):
    half = HEAD // 2
    freq = (float(THETA) ** (-np.arange(half, dtype=np.float64) / half)).astype(np.float32)[None]

    def step(x, gain, wq, wk, wv, wo):
        rows, wide = x.shape
        deep, width = wq.shape
        vmem, hbm = pl.BlockSpec(memory_space=pltpu.VMEM), pl.BlockSpec(memory_space=pltpu.HBM)
        dma = pltpu.SemaphoreType.DMA
        return pl.pallas_call(
            kernel,
            out_shape=jax.ShapeDtypeStruct((rows, wide), BF16),
            in_specs=[hbm, vmem, vmem] + [hbm] * 4,
            out_specs=hbm,
            scratch_shapes=[
                pltpu.VMEM((4, 4, 2, deep, width), BF16),
                pltpu.VMEM((4, 4, 2, deep, wide), BF16),
                pltpu.VMEM((4, 4, 2, deep, 2 * HEAD), BF16),
                pltpu.VMEM((4, 4, 2, 2 * HEAD, HEAD), BF16),
                pltpu.VMEM((rows, wide), BF16),
                pltpu.VMEM((rows, wide), BF16),
                pltpu.VMEM((4, 4, rows, 2 * deep), BF16),
                pltpu.VMEM((HEAD, width), BF16),
                pltpu.VMEM((HEAD + 8, width), F32),
                pltpu.VMEM((rows, wide), F32),
                pltpu.VMEM((8, width), F32),
                pltpu.VMEM((rows, half), F32),
                pltpu.VMEM((rows, half), F32),
                dma((5,)),
                dma((2,)),
                *[dma((4, 4))] * 11,
                *[dma((4, 16))] * 2,
                *[dma((4, 4))] * 7,
            ],
            compiler_params=pltpu.CompilerParams(collective_id=0, has_side_effects=True, vmem_limit_bytes=63 * 2**20),
        )(x, gain, jnp.asarray(freq), wq, wk, wv, wo)

    tokens, whole = P(("dp", "sp"), None), P("sp", None)
    return jax.shard_map(step, mesh=mesh, in_specs=(tokens, P(None), whole, whole, whole, whole), out_specs=tokens, check_vma=False)
```

```python
import functools

import jax
import jax.numpy as jnp
import numpy as np
from jax import lax
from jax.experimental import pallas as pl
from jax.experimental.pallas import tpu as pltpu
from jax.sharding import PartitionSpec as P

HEAD = 256
THETA = 10000
LOG2E = 1.4426950408889634
HIDDEN = -1e30
MESH = pl.DeviceIdType.MESH
F32, BF16 = jnp.float32, jnp.bfloat16
WKV, WQ, KV, WO = range(4)

STAGES = (
    ((0, 0),),
    ((1, 0), (0, 1), (0, 2)),
    ((2, 0), (1, 1), (1, 2), (0, 3)),
    ((3, 0), (2, 1), (2, 2), (1, 3)),
    ((3, 1), (3, 2), (2, 3)),
    ((3, 3),),
)
MAIN, A, B, LATE, LATE_A, LATE_B = range(6)
CUTS = {
    WKV: (1, ((0, 512), (0, 256), (256, 256), None, None, None)),
    WQ: (1, ((0, 1408), (0, 640), (640, 768), (1408, 640), (1408, 384), (1792, 256))),
    KV: (0, ((0, 400), (0, 192), (192, 208), (400, 112), (400, 64), (464, 48))),
    WO: (1, ((0, 1792), (0, 896), (896, 896), (1792, 256), (1792, 128), (1920, 128))),
}


WORK = {1: ((KV, 3),), 3: ((WO, 2),), 7: ((KV, 4),), 10: ((WO, 3),), 11: ((KV, 5),), 14: ((WO, 4),)}


def dot(a, b):
    return jnp.dot(a, b, preferred_element_type=F32)


def kernel(x_hbm, gain_hbm, freq_hbm, wq_ref, wk_ref, wv_ref, wo_ref, out_hbm,
           wqb, wob, wkvb, kvb, x_ref, gain_ref, freq_ref, out_ref, a_s, qt_s, mix_s, acc_s, top_s, cos_s, sin_s,
           local_sem, out_sem, up_s, down_s, z_r, x_s, x_r, y_s, y_r, ha_s, ha_r, hb_s, hb_r, p_s, p_r,
           late_s, late_r, late_up_s, late_down_s, late_z_r, late_p_s, late_p_r):
    me = lax.axis_index("sp")
    core, chip = lax.rem(me, 2), lax.div(me, 2)
    z, y, x = lax.rem(chip, 4), lax.rem(lax.div(chip, 4), 2), lax.div(chip, 8)
    ranks = (z, z + 1 - 2 * lax.rem(z, 2), jnp.where(z >= 2, 1, 2), jnp.where(z >= 2, 0, 3))
    columns = (x * 2 + y, x * 2 + 1 - y, (1 - x) * 2 + y, (1 - x) * 2 + 1 - y)
    above, below, partner = me + 2, me - 2, me + 1 - 2 * core
    x_peer, y_peer = columns[2] * 8 + z * 2 + core, columns[1] * 8 + z * 2 + core
    bufs = (wkvb, wqb, kvb, wob)

    def remote(src, send_sem, recv_sem, to):
        return pltpu.make_async_remote_copy(src_ref=src, dst_ref=src, send_sem=send_sem, recv_sem=recv_sem, device_id={"sp": to}, device_id_type=MESH)

    def given(when, do):
        if when is None:
            do()
        else:
            pl.when(when)(do)

    def arrived(ref, recv_sem):
        pltpu.make_async_remote_copy(src_ref=ref, dst_ref=ref, send_sem=recv_sem, recv_sem=recv_sem, device_id={"sp": partner}, device_id_type=MESH).wait_recv()

    def piece(u, r, q, c, which):
        axis, cuts = CUTS[u]
        start, size = cuts[which]
        column = slice(None) if q is None else columns[q]
        here = pl.ds(start, size)
        return bufs[u].at[column, ranks[r], c, here] if axis == 0 else bufs[u].at[column, ranks[r], c, :, here]

    def sends(u, r, q):
        ref = piece(u, r, q, core, MAIN)
        copies = [(remote(ref, p_s.at[u, 4 * q + r], p_r.at[u, 4 * q + r], partner), None)]
        if q == 0:
            at = ranks[r]
            copies = [
                (remote(ref, up_s.at[u, r], z_r.at[u, at], above), (at <= z) & (z < 3)),
                (remote(ref, down_s.at[u, r], z_r.at[u, at], below), (at >= z) & (z > 0)),
                (remote(ref, x_s.at[u, r], x_r.at[u, r], x_peer), None),
                (remote(ref, y_s.at[u, r], y_r.at[u, r], y_peer), None),
            ] + copies
        elif q == 1:
            copies = [(remote(piece(u, r, q, core, B), hb_s.at[u, r], hb_r.at[u, r], x_peer), None)] + copies
        elif q == 2:
            copies = [(remote(piece(u, r, q, core, A), ha_s.at[u, r], ha_r.at[u, r], y_peer), None)] + copies
        return copies

    def event(u, r, q):
        if q == 0 and r:
            arrived(piece(u, r, q, core, MAIN), z_r.at[u, ranks[r]])
        elif q == 1:
            arrived(piece(u, r, q, core, MAIN), y_r.at[u, r])
        elif q == 2:
            arrived(piece(u, r, q, core, MAIN), x_r.at[u, r])
        elif q == 3:
            arrived(piece(u, r, q, core, A), ha_r.at[u, r])
            arrived(piece(u, r, q, core, B), hb_r.at[u, r])
        for copy, when in sends(u, r, q):
            given(when, copy.start)

    def late_sends(u, n):
        if n == 0:
            ref = piece(u, 0, 0, core, LATE)
            return [(remote(ref, late_s.at[u, 0], late_r.at[u, 0], x_peer), None), (remote(ref, late_s.at[u, 1], late_r.at[u, 1], y_peer), None)]
        if n == 1:
            copies = [(remote(piece(u, 0, 2, core, LATE_A), late_s.at[u, 2], late_r.at[u, 2], y_peer), None)]
            if CUTS[u][1][LATE_B]:
                copies.append((remote(piece(u, 0, 1, core, LATE_B), late_s.at[u, 3], late_r.at[u, 3], x_peer), None))
            return copies
        r = n - 2
        at, ref = ranks[r], piece(u, r, None, core, LATE)
        return [
            (remote(ref, late_up_s.at[u, r], late_z_r.at[u, at], above), (at <= z) & (z < 3)),
            (remote(ref, late_down_s.at[u, r], late_z_r.at[u, at], below), (at >= z) & (z > 0)),
            (remote(ref, late_p_s.at[u, r], late_p_r.at[u, r], partner), None),
        ]

    def late_event(u, n):
        if n == 1:
            arrived(piece(u, 0, 2, core, LATE), late_r.at[u, 0])
            arrived(piece(u, 0, 1, core, LATE), late_r.at[u, 1])
        elif n == 2:
            arrived(piece(u, 0, 3, core, LATE_A), late_r.at[u, 2])
            if CUTS[u][1][LATE_B]:
                arrived(piece(u, 0, 3, core, LATE_B), late_r.at[u, 3])
        elif n > 2:
            arrived(piece(u, n - 2, None, core, LATE), late_z_r.at[u, ranks[n - 2]])
        for copy, when in late_sends(u, n):
            given(when, copy.start)

    def stage(u, n):
        if u != WKV:
            late_event(u, n)
        for r, q in STAGES[n]:
            event(u, r, q)

    def other(u, r, q):
        arrived(piece(u, r, q, 1 - core, MAIN), p_r.at[u, 4 * q + r])
        if u != WKV and q == 0:
            arrived(piece(u, r, None, 1 - core, LATE), late_p_r.at[u, r])

    def others(u):
        for r in range(4):
            for q in range(4):
                other(u, r, q)

    own = [
        pltpu.make_async_copy(wk_ref, wkvb.at[columns[0], z, core, :, pl.ds(0, HEAD)], local_sem.at[0]),
        pltpu.make_async_copy(wv_ref, wkvb.at[columns[0], z, core, :, pl.ds(HEAD, HEAD)], local_sem.at[1]),
        pltpu.make_async_copy(wq_ref, wqb.at[columns[0], z, core], local_sem.at[2]),
        pltpu.make_async_copy(wo_ref, wob.at[columns[0], z, core], local_sem.at[3]),
        pltpu.make_async_copy(x_hbm, x_ref, local_sem.at[4]),
        pltpu.make_async_copy(gain_hbm, gain_ref, local_sem.at[5]),
        pltpu.make_async_copy(freq_hbm, freq_ref, local_sem.at[6]),
    ]

    barrier = pltpu.get_barrier_semaphore()

    def greet(to):
        pl.semaphore_signal(barrier, inc=1, device_id={"sp": to}, device_id_type=MESH)

    for to in (x_peer, y_peer, partner):
        greet(to)
    pl.when(z < 3)(lambda: greet(above))
    pl.when(z > 0)(lambda: greet(below))
    for copy in own:
        copy.start()
    pl.semaphore_wait(barrier, jnp.where((z > 0) & (z < 3), 5, 4))

    rows, wide = x_ref.shape
    heads = wide // HEAD

    def normalise():
        for copy in own[4:]:
            copy.wait()
        gain = gain_ref[...].astype(F32).reshape(1, -1)

        @pl.loop(0, rows // 64)
        def _(n):
            here = pl.ds(n * 64, 64)
            wide = x_ref[here, :].astype(F32)
            scale = lax.rsqrt(jnp.mean(wide * wide, -1, keepdims=True) + 1e-6)
            a = (wide * scale * gain).astype(BF16)
            for i in range(16):
                a_s[i // 4, i % 4, here, :] = a[:, i * 128 : (i + 1) * 128]

        place = (me * rows + lax.broadcasted_iota(jnp.int32, (rows, HEAD // 2), 0)).astype(F32)
        angle = place * freq_ref[...]
        cos_s[...] = jnp.cos(angle)
        sin_s[...] = jnp.sin(angle)

    def turned(t):
        t = t.astype(BF16).astype(F32)
        a, b, cos, sin = t[:, : HEAD // 2], t[:, HEAD // 2 :], cos_s[...], sin_s[...]
        return jnp.concatenate([a * cos - b * sin, b * cos + a * sin], -1)

    def strip_of(ref, ranks_in):
        return jnp.concatenate([ref[q, r] for r in ranks_in for q in range(4)], axis=1)

    def partial(ref, weights, ranks_in, into, first):
        left = strip_of(ref, ranks_in)

        @pl.loop(0, wide // 512)
        def _(n):
            cols = pl.ds(pl.multiple_of(n * 512, 512), 512)
            right = jnp.concatenate([weights[:, r, :, :, cols].reshape(-1, 512) for r in ranks_in], axis=0)
            got = dot(left, right)
            into[0:rows, cols] = got if first else into[0:rows, cols] + got

    def rank_in(u, r):
        for q in range(4):
            other(u, r, q)

    def query(n, first=False):
        rank_in(WQ, n)
        partial(a_s, wqb, [ranks[n]], mix_s, first)

    def keys_values():
        others(WKV)
        kv = dot(strip_of(a_s, range(4)), jnp.concatenate([wkvb[:, r].reshape(-1, 2 * HEAD) for r in range(4)], axis=0))
        kvb[columns[0], z, core, 0:HEAD, :] = turned(kv[:, :HEAD]).astype(BF16)
        kvb[columns[0], z, core, HEAD:, :] = kv[:, HEAD:].astype(BF16).astype(F32).T.astype(BF16)

    def queries_turned():
        @pl.loop(0, heads)
        def _(h):
            cols = pl.ds(pl.multiple_of(h * HEAD, HEAD), HEAD)
            qt_s[:, cols] = turned(mix_s[0:rows, cols]).T.astype(BF16)

    own[0].wait()
    own[1].wait()
    stage(WKV, 0)
    own[2].wait()
    stage(WQ, 0)
    normalise()
    for u, n in ((WKV, 1), (WKV, 2), (WKV, 3), (WQ, 1)):
        stage(u, n)
    own[3].wait()
    for u, n in ((WO, 0), (WKV, 4), (WQ, 2), (WKV, 5)):
        stage(u, n)
    keys_values()
    stage(KV, 0)
    query(0, True)
    for u, n in ((WQ, 3), (KV, 1), (WQ, 4), (KV, 2), (WO, 1)):
        stage(u, n)
    query(1)
    stage(WQ, 5)
    query(2)
    query(3)
    queries_turned()

    e = HEAD**-0.5 * LOG2E
    width = qt_s.shape[1]
    strip = 512
    strips = range(0, width, strip)
    keys = 2 * rows
    ones = jnp.ones((8, keys), BF16)

    def step(column, at, masked):
        k = kvb[column, at, :, 0:HEAD, :].reshape(keys, HEAD)
        v = jnp.concatenate([kvb[column, at, 0, HEAD:, :], kvb[column, at, 1, HEAD:, :]], axis=1)
        v = jnp.concatenate([v, ones], axis=0)
        scores = [dot(k, qt_s[:, n : n + strip]) for n in strips]
        weights, keeps = [], []
        for n, s in zip(strips, scores):
            if masked:
                ahead = lax.rem(lax.broadcasted_iota(jnp.int32, s.shape, 1), rows) - lax.broadcasted_iota(jnp.int32, s.shape, 0)
                s = jnp.where(ahead >= -rows * core, s, HIDDEN)
                top = s.max(axis=0, keepdims=True)
            else:
                old = top_s[0:1, n : n + strip]
                top = jnp.maximum(old, s.max(axis=0, keepdims=True))
                keeps.append(jnp.exp2((old - top) * e))
            top_s[0:1, n : n + strip] = top
            weights.append(jnp.exp2((s - top) * e).astype(BF16))
        for i, n in enumerate(strips):
            add = dot(v, weights[i])
            mix_s[:, n : n + strip] = add if masked else mix_s[:, n : n + strip] * keeps[i] + add

    other(KV, 0, 0)
    step(columns[0], z, True)

    @pl.loop(1, 16)
    def _(i):
        def at(n, *todo):
            @pl.when(i == n)
            def _():
                for do in todo:
                    do()

        for r in range(4):
            for q in range(4):
                n = 4 * r + q
                todo = []
                for u, m in WORK.get(n, ()):
                    todo.append(functools.partial(stage, u, m))
                if n:
                    todo.append(functools.partial(other, KV, r, q))
                    at(n, *todo)

        r, q = lax.div(i, 4), lax.rem(i, 4)
        rank = jnp.where(r == 0, ranks[0], jnp.where(r == 1, ranks[1], jnp.where(r == 2, ranks[2], ranks[3])))
        column = jnp.where(q == 0, columns[0], jnp.where(q == 1, columns[1], jnp.where(q == 2, columns[2], columns[3])))

        @pl.when(column * 4 + rank < chip)
        def _():
            step(column, rank, False)

    def attended():
        @pl.loop(0, heads)
        def _(h):
            cols = pl.ds(pl.multiple_of(h * HEAD, HEAD), HEAD)
            o = (mix_s[0:HEAD, cols] * (1 / mix_s[HEAD : HEAD + 1, cols])).T.astype(BF16)
            column, at = lax.div(h, 2), 2 * lax.rem(h, 2)
            a_s[column, at] = o[:, : HEAD // 2]
            a_s[column, at + 1] = o[:, HEAD // 2 :]

    stores = []

    def finish(left, ranks_in, start, first, last):
        for n in range(start, start + 1024, 512):
            cols = pl.ds(n, 512)
            got = dot(left, jnp.concatenate([wob[:, r, :, :, cols].reshape(-1, 512) for r in ranks_in], axis=0))
            if not first:
                got = acc_s[:, cols] + got
            if last:
                out_ref[:, cols] = (x_ref[:, cols].astype(F32) + got).astype(BF16)
                stores.append(pltpu.make_async_copy(out_ref.at[:, cols], out_hbm.at[:, cols], out_sem.at[len(stores)]))
                stores[-1].start()
            else:
                acc_s[:, cols] = got

    for u in (WKV, WQ):
        copies = [copy for r in range(4) for q in range(4) for copy in sends(u, r, q)]
        if u != WKV:
            copies += [copy for n in range(6) for copy in late_sends(u, n)]
        for copy, when in copies:
            given(when, copy.wait_send)
    attended()
    stage(WO, 5)
    for r in range(3):
        rank_in(WO, r)
    for at in (0, 1024):
        finish(strip_of(a_s, ranks[:3]), ranks[:3], at, True, False)
    rank_in(WO, 3)
    for at in (0, 1024):
        finish(strip_of(a_s, ranks[3:]), ranks[3:], at, False, True)
    for copy in stores:
        copy.wait()

    for u in (KV, WO):
        copies = [copy for r in range(4) for q in range(4) for copy in sends(u, r, q)]
        if u != WKV:
            copies += [copy for n in range(6) for copy in late_sends(u, n)]
        for copy, when in copies:
            given(when, copy.wait_send)


def solution(mesh):
    half = HEAD // 2
    freq = (float(THETA) ** (-np.arange(half, dtype=np.float64) / half)).astype(np.float32)[None]

    def step(x, gain, wq, wk, wv, wo):
        rows, wide = x.shape
        deep, width = wq.shape
        hbm = pl.BlockSpec(memory_space=pltpu.HBM)
        dma = pltpu.SemaphoreType.DMA
        return pl.pallas_call(
            kernel,
            out_shape=jax.ShapeDtypeStruct((rows, wide), BF16),
            in_specs=[hbm] * 7,
            out_specs=hbm,
            scratch_shapes=[
                pltpu.VMEM((4, 4, 2, deep, width), BF16),
                pltpu.VMEM((4, 4, 2, deep, wide), BF16),
                pltpu.VMEM((4, 4, 2, deep, 2 * HEAD), BF16),
                pltpu.VMEM((4, 4, 2, 2 * HEAD, HEAD), BF16),
                pltpu.VMEM((rows, wide), BF16),
                pltpu.VMEM((wide,), BF16),
                pltpu.VMEM((1, half), F32),
                pltpu.VMEM((rows, wide), BF16),
                pltpu.VMEM((4, 4, rows, 2 * deep), BF16),
                pltpu.VMEM((HEAD, width), BF16),
                pltpu.VMEM((HEAD + 8, width), F32),
                pltpu.VMEM((rows, wide), F32),
                pltpu.VMEM((8, width), F32),
                pltpu.VMEM((rows, half), F32),
                pltpu.VMEM((rows, half), F32),
                dma((7,)),
                dma((4,)),
                *[dma((4, 4))] * 11,
                *[dma((4, 16))] * 2,
                *[dma((4, 4))] * 7,
            ],
            compiler_params=pltpu.CompilerParams(collective_id=0, has_side_effects=True, vmem_limit_bytes=63 * 2**20),
        )(x, gain, jnp.asarray(freq), wq, wk, wv, wo)

    tokens, whole = P(("dp", "sp"), None), P("sp", None)
    return jax.shard_map(step, mesh=mesh, in_specs=(tokens, P(None), whole, whole, whole, whole), out_specs=tokens, check_vma=False)
```

```python
import functools

import jax
import jax.numpy as jnp
import numpy as np
from jax import lax
from jax.experimental import pallas as pl
from jax.experimental.pallas import tpu as pltpu
from jax.sharding import PartitionSpec as P

HEAD = 256
THETA = 10000
LOG2E = 1.4426950408889634
HIDDEN = -1e30
MESH = pl.DeviceIdType.MESH
F32, BF16 = jnp.float32, jnp.bfloat16
WKV, WQ, KV, WO = range(4)

STAGES = (
    ((0, 0),),
    ((1, 0), (0, 1), (0, 2)),
    ((2, 0), (1, 1), (1, 2), (0, 3)),
    ((3, 0), (2, 1), (2, 2), (1, 3)),
    ((3, 1), (3, 2), (2, 3)),
    ((3, 3),),
)
MAIN, A, B, LATE, LATE_A, LATE_B = range(6)
CUTS = {
    WKV: (1, ((0, 512), (0, 256), (256, 256), None, None, None)),
    WQ: (1, ((0, 1408), (0, 640), (640, 768), (1408, 640), (1408, 384), (1792, 256))),
    KV: (0, ((0, 400), (0, 192), (192, 208), (400, 112), (400, 64), (464, 48))),
    WO: (1, ((0, 1792), (0, 896), (896, 896), (1792, 256), (1792, 128), (1920, 128))),
}


WORK = {1: ((KV, 3),), 3: ((WO, 2),), 7: ((KV, 4),), 10: ((WO, 3),), 11: ((KV, 5),), 14: ((WO, 4),)}


def dot(a, b):
    return jnp.dot(a, b, preferred_element_type=F32)


def kernel(x_hbm, gain_hbm, freq_hbm, wq_ref, wk_ref, wv_ref, wo_ref, out_hbm,
           wqb, wob, wkvb, kvb, x_ref, gain_ref, freq_ref, out_ref, a_s, qt_s, mix_s, acc_s, top_s, cos_s, sin_s,
           local_sem, out_sem, up_s, down_s, z_r, x_s, x_r, y_s, y_r, ha_s, ha_r, hb_s, hb_r, p_s, p_r,
           late_s, late_r, late_up_s, late_down_s, late_z_r, late_p_s, late_p_r):
    me = lax.axis_index("sp")
    core, chip = lax.rem(me, 2), lax.div(me, 2)
    z, y, x = lax.rem(chip, 4), lax.rem(lax.div(chip, 4), 2), lax.div(chip, 8)
    ranks = (z, z + 1 - 2 * lax.rem(z, 2), jnp.where(z >= 2, 1, 2), jnp.where(z >= 2, 0, 3))
    columns = (x * 2 + y, x * 2 + 1 - y, (1 - x) * 2 + y, (1 - x) * 2 + 1 - y)
    above, below, partner = me + 2, me - 2, me + 1 - 2 * core
    x_peer, y_peer = columns[2] * 8 + z * 2 + core, columns[1] * 8 + z * 2 + core
    bufs = (wkvb, wqb, kvb, wob)

    def remote(src, send_sem, recv_sem, to):
        return pltpu.make_async_remote_copy(src_ref=src, dst_ref=src, send_sem=send_sem, recv_sem=recv_sem, device_id={"sp": to}, device_id_type=MESH)

    def given(when, do):
        if when is None:
            do()
        else:
            pl.when(when)(do)

    def arrived(ref, recv_sem):
        pltpu.make_async_remote_copy(src_ref=ref, dst_ref=ref, send_sem=recv_sem, recv_sem=recv_sem, device_id={"sp": partner}, device_id_type=MESH).wait_recv()

    def piece(u, r, q, c, which):
        axis, cuts = CUTS[u]
        start, size = cuts[which]
        column = slice(None) if q is None else columns[q]
        here = pl.ds(start, size)
        return bufs[u].at[column, ranks[r], c, here] if axis == 0 else bufs[u].at[column, ranks[r], c, :, here]

    def sends(u, r, q):
        ref = piece(u, r, q, core, MAIN)
        copies = [(remote(ref, p_s.at[u, 4 * q + r], p_r.at[u, 4 * q + r], partner), None)]
        if q == 0:
            at = ranks[r]
            copies = [
                (remote(ref, up_s.at[u, r], z_r.at[u, at], above), (at <= z) & (z < 3)),
                (remote(ref, down_s.at[u, r], z_r.at[u, at], below), (at >= z) & (z > 0)),
                (remote(ref, x_s.at[u, r], x_r.at[u, r], x_peer), None),
                (remote(ref, y_s.at[u, r], y_r.at[u, r], y_peer), None),
            ] + copies
        elif q == 1:
            copies = [(remote(piece(u, r, q, core, B), hb_s.at[u, r], hb_r.at[u, r], x_peer), None)] + copies
        elif q == 2:
            copies = [(remote(piece(u, r, q, core, A), ha_s.at[u, r], ha_r.at[u, r], y_peer), None)] + copies
        return copies

    def event(u, r, q):
        if q == 0 and r:
            arrived(piece(u, r, q, core, MAIN), z_r.at[u, ranks[r]])
        elif q == 1:
            arrived(piece(u, r, q, core, MAIN), y_r.at[u, r])
        elif q == 2:
            arrived(piece(u, r, q, core, MAIN), x_r.at[u, r])
        elif q == 3:
            arrived(piece(u, r, q, core, A), ha_r.at[u, r])
            arrived(piece(u, r, q, core, B), hb_r.at[u, r])
        for copy, when in sends(u, r, q):
            given(when, copy.start)

    def late_sends(u, n):
        if n == 0:
            ref = piece(u, 0, 0, core, LATE)
            return [(remote(ref, late_s.at[u, 0], late_r.at[u, 0], x_peer), None), (remote(ref, late_s.at[u, 1], late_r.at[u, 1], y_peer), None)]
        if n == 1:
            copies = [(remote(piece(u, 0, 2, core, LATE_A), late_s.at[u, 2], late_r.at[u, 2], y_peer), None)]
            if CUTS[u][1][LATE_B]:
                copies.append((remote(piece(u, 0, 1, core, LATE_B), late_s.at[u, 3], late_r.at[u, 3], x_peer), None))
            return copies
        r = n - 2
        at, ref = ranks[r], piece(u, r, None, core, LATE)
        return [
            (remote(ref, late_up_s.at[u, r], late_z_r.at[u, at], above), (at <= z) & (z < 3)),
            (remote(ref, late_down_s.at[u, r], late_z_r.at[u, at], below), (at >= z) & (z > 0)),
            (remote(ref, late_p_s.at[u, r], late_p_r.at[u, r], partner), None),
        ]

    def late_event(u, n):
        if n == 1:
            arrived(piece(u, 0, 2, core, LATE), late_r.at[u, 0])
            arrived(piece(u, 0, 1, core, LATE), late_r.at[u, 1])
        elif n == 2:
            arrived(piece(u, 0, 3, core, LATE_A), late_r.at[u, 2])
            if CUTS[u][1][LATE_B]:
                arrived(piece(u, 0, 3, core, LATE_B), late_r.at[u, 3])
        elif n > 2:
            arrived(piece(u, n - 2, None, core, LATE), late_z_r.at[u, ranks[n - 2]])
        for copy, when in late_sends(u, n):
            given(when, copy.start)

    def stage(u, n):
        if u != WKV:
            late_event(u, n)
        for r, q in STAGES[n]:
            event(u, r, q)

    def other(u, r, q):
        arrived(piece(u, r, q, 1 - core, MAIN), p_r.at[u, 4 * q + r])
        if u != WKV and q == 0:
            arrived(piece(u, r, None, 1 - core, LATE), late_p_r.at[u, r])

    def others(u):
        for r in range(4):
            for q in range(4):
                other(u, r, q)

    own = [
        pltpu.make_async_copy(wk_ref, wkvb.at[columns[0], z, core, :, pl.ds(0, HEAD)], local_sem.at[0]),
        pltpu.make_async_copy(wv_ref, wkvb.at[columns[0], z, core, :, pl.ds(HEAD, HEAD)], local_sem.at[1]),
        pltpu.make_async_copy(wq_ref, wqb.at[columns[0], z, core], local_sem.at[2]),
        pltpu.make_async_copy(wo_ref, wob.at[columns[0], z, core], local_sem.at[3]),
        pltpu.make_async_copy(x_hbm, x_ref, local_sem.at[4]),
        pltpu.make_async_copy(gain_hbm, gain_ref, local_sem.at[5]),
        pltpu.make_async_copy(freq_hbm, freq_ref, local_sem.at[6]),
    ]

    barrier = pltpu.get_barrier_semaphore()

    def greet(to):
        pl.semaphore_signal(barrier, inc=1, device_id={"sp": to}, device_id_type=MESH)

    for to in (x_peer, y_peer, partner):
        greet(to)
    pl.when(z < 3)(lambda: greet(above))
    pl.when(z > 0)(lambda: greet(below))
    for copy in own:
        copy.start()
    pl.semaphore_wait(barrier, jnp.where((z > 0) & (z < 3), 5, 4))

    rows, wide = x_ref.shape
    heads = wide // HEAD

    def normalise():
        for copy in own[4:]:
            copy.wait()
        gain = gain_ref[...].astype(F32).reshape(1, -1)

        @pl.loop(0, rows // 64)
        def _(n):
            here = pl.ds(n * 64, 64)
            wide = x_ref[here, :].astype(F32)
            scale = lax.rsqrt(jnp.mean(wide * wide, -1, keepdims=True) + 1e-6)
            a = (wide * scale * gain).astype(BF16)
            for i in range(16):
                a_s[i // 4, i % 4, here, :] = a[:, i * 128 : (i + 1) * 128]

        place = (me * rows + lax.broadcasted_iota(jnp.int32, (rows, HEAD // 2), 0)).astype(F32)
        angle = place * freq_ref[...]
        cos_s[...] = jnp.cos(angle)
        sin_s[...] = jnp.sin(angle)

    def turned(t):
        t = t.astype(BF16).astype(F32)
        a, b, cos, sin = t[:, : HEAD // 2], t[:, HEAD // 2 :], cos_s[...], sin_s[...]
        return jnp.concatenate([a * cos - b * sin, b * cos + a * sin], -1)

    def strip_of(ref, ranks_in):
        return jnp.concatenate([ref[q, r] for r in ranks_in for q in range(4)], axis=1)

    def partial(ref, weights, ranks_in, into, first):
        left = strip_of(ref, ranks_in)

        @pl.loop(0, wide // 512)
        def _(n):
            cols = pl.ds(pl.multiple_of(n * 512, 512), 512)
            right = jnp.concatenate([weights[:, r, :, :, cols].reshape(-1, 512) for r in ranks_in], axis=0)
            got = dot(left, right)
            into[0:rows, cols] = got if first else into[0:rows, cols] + got

    def rank_in(u, r):
        for q in range(4):
            other(u, r, q)

    def query(n, first=False):
        rank_in(WQ, n)
        partial(a_s, wqb, [ranks[n]], mix_s, first)

    def keys_values():
        others(WKV)
        kv = dot(strip_of(a_s, range(4)), jnp.concatenate([wkvb[:, r].reshape(-1, 2 * HEAD) for r in range(4)], axis=0))
        kvb[columns[0], z, core, 0:HEAD, :] = turned(kv[:, :HEAD]).astype(BF16)
        kvb[columns[0], z, core, HEAD:, :] = kv[:, HEAD:].astype(BF16).astype(F32).T.astype(BF16)

    def queries_turned():
        @pl.loop(0, heads)
        def _(h):
            cols = pl.ds(pl.multiple_of(h * HEAD, HEAD), HEAD)
            qt_s[:, cols] = turned(mix_s[0:rows, cols]).T.astype(BF16)

    own[0].wait()
    own[1].wait()
    stage(WKV, 0)
    normalise()
    own[2].wait()
    stage(WQ, 0)
    for u, n in ((WKV, 1), (WKV, 2), (WKV, 3), (WQ, 1)):
        stage(u, n)
    own[3].wait()
    for u, n in ((WO, 0), (WKV, 4), (WQ, 2), (WKV, 5)):
        stage(u, n)
    keys_values()
    stage(KV, 0)
    query(0, True)
    for u, n in ((WQ, 3), (KV, 1), (WQ, 4), (KV, 2), (WO, 1)):
        stage(u, n)
    query(1)
    stage(WQ, 5)
    query(2)
    query(3)
    queries_turned()

    e = HEAD**-0.5 * LOG2E
    width = qt_s.shape[1]
    strip = 512
    strips = range(0, width, strip)
    keys = 2 * rows
    ones = jnp.ones((8, keys), BF16)

    def step(column, at, masked):
        k = kvb[column, at, :, 0:HEAD, :].reshape(keys, HEAD)
        v = jnp.concatenate([kvb[column, at, 0, HEAD:, :], kvb[column, at, 1, HEAD:, :]], axis=1)
        v = jnp.concatenate([v, ones], axis=0)
        scores = [dot(k, qt_s[:, n : n + strip]) for n in strips]
        weights, keeps = [], []
        for n, s in zip(strips, scores):
            if masked:
                ahead = lax.rem(lax.broadcasted_iota(jnp.int32, s.shape, 1), rows) - lax.broadcasted_iota(jnp.int32, s.shape, 0)
                s = jnp.where(ahead >= -rows * core, s, HIDDEN)
                top = s.max(axis=0, keepdims=True)
            else:
                old = top_s[0:1, n : n + strip]
                top = jnp.maximum(old, s.max(axis=0, keepdims=True))
                keeps.append(jnp.exp2((old - top) * e))
            top_s[0:1, n : n + strip] = top
            weights.append(jnp.exp2((s - top) * e).astype(BF16))
        for i, n in enumerate(strips):
            add = dot(v, weights[i])
            mix_s[:, n : n + strip] = add if masked else mix_s[:, n : n + strip] * keeps[i] + add

    other(KV, 0, 0)
    step(columns[0], z, True)

    @pl.loop(1, 16)
    def _(i):
        def at(n, *todo):
            @pl.when(i == n)
            def _():
                for do in todo:
                    do()

        for r in range(4):
            for q in range(4):
                n = 4 * r + q
                todo = []
                for u, m in WORK.get(n, ()):
                    todo.append(functools.partial(stage, u, m))
                if n:
                    todo.append(functools.partial(other, KV, r, q))
                    at(n, *todo)

        r, q = lax.div(i, 4), lax.rem(i, 4)
        rank = jnp.where(r == 0, ranks[0], jnp.where(r == 1, ranks[1], jnp.where(r == 2, ranks[2], ranks[3])))
        column = jnp.where(q == 0, columns[0], jnp.where(q == 1, columns[1], jnp.where(q == 2, columns[2], columns[3])))

        @pl.when(column * 4 + rank < chip)
        def _():
            step(column, rank, False)

    def attended():
        @pl.loop(0, heads)
        def _(h):
            cols = pl.ds(pl.multiple_of(h * HEAD, HEAD), HEAD)
            o = (mix_s[0:HEAD, cols] * (1 / mix_s[HEAD : HEAD + 1, cols])).T.astype(BF16)
            column, at = lax.div(h, 2), 2 * lax.rem(h, 2)
            a_s[column, at] = o[:, : HEAD // 2]
            a_s[column, at + 1] = o[:, HEAD // 2 :]

    stores = []

    def finish(left, ranks_in, start, first, last):
        for n in range(start, start + 1024, 512):
            cols = pl.ds(n, 512)
            got = dot(left, jnp.concatenate([wob[:, r, :, :, cols].reshape(-1, 512) for r in ranks_in], axis=0))
            if not first:
                got = acc_s[:, cols] + got
            if last:
                out_ref[:, cols] = (x_ref[:, cols].astype(F32) + got).astype(BF16)
                stores.append(pltpu.make_async_copy(out_ref.at[:, cols], out_hbm.at[:, cols], out_sem.at[len(stores)]))
                stores[-1].start()
            else:
                acc_s[:, cols] = got

    for u in (WKV, WQ):
        copies = [copy for r in range(4) for q in range(4) for copy in sends(u, r, q)]
        if u != WKV:
            copies += [copy for n in range(6) for copy in late_sends(u, n)]
        for copy, when in copies:
            given(when, copy.wait_send)
    attended()
    stage(WO, 5)
    for r in range(3):
        rank_in(WO, r)
    for at in (0, 1024):
        finish(strip_of(a_s, ranks[:3]), ranks[:3], at, True, False)
    rank_in(WO, 3)
    for at in (0, 1024):
        finish(strip_of(a_s, ranks[3:]), ranks[3:], at, False, True)
    for copy in stores:
        copy.wait()

    for u in (KV, WO):
        copies = [copy for r in range(4) for q in range(4) for copy in sends(u, r, q)]
        if u != WKV:
            copies += [copy for n in range(6) for copy in late_sends(u, n)]
        for copy, when in copies:
            given(when, copy.wait_send)


def solution(mesh):
    half = HEAD // 2
    freq = (float(THETA) ** (-np.arange(half, dtype=np.float64) / half)).astype(np.float32)[None]

    def step(x, gain, wq, wk, wv, wo):
        rows, wide = x.shape
        deep, width = wq.shape
        hbm = pl.BlockSpec(memory_space=pltpu.HBM)
        dma = pltpu.SemaphoreType.DMA
        return pl.pallas_call(
            kernel,
            out_shape=jax.ShapeDtypeStruct((rows, wide), BF16),
            in_specs=[hbm] * 7,
            out_specs=hbm,
            scratch_shapes=[
                pltpu.VMEM((4, 4, 2, deep, width), BF16),
                pltpu.VMEM((4, 4, 2, deep, wide), BF16),
                pltpu.VMEM((4, 4, 2, deep, 2 * HEAD), BF16),
                pltpu.VMEM((4, 4, 2, 2 * HEAD, HEAD), BF16),
                pltpu.VMEM((rows, wide), BF16),
                pltpu.VMEM((wide,), BF16),
                pltpu.VMEM((1, half), F32),
                pltpu.VMEM((rows, wide), BF16),
                pltpu.VMEM((4, 4, rows, 2 * deep), BF16),
                pltpu.VMEM((HEAD, width), BF16),
                pltpu.VMEM((HEAD + 8, width), F32),
                pltpu.VMEM((rows, wide), F32),
                pltpu.VMEM((8, width), F32),
                pltpu.VMEM((rows, half), F32),
                pltpu.VMEM((rows, half), F32),
                dma((7,)),
                dma((4,)),
                *[dma((4, 4))] * 11,
                *[dma((4, 16))] * 2,
                *[dma((4, 4))] * 7,
            ],
            compiler_params=pltpu.CompilerParams(collective_id=0, has_side_effects=True, vmem_limit_bytes=63 * 2**20),
        )(x, gain, jnp.asarray(freq), wq, wk, wv, wo)

    tokens, whole = P(("dp", "sp"), None), P("sp", None)
    return jax.shard_map(step, mesh=mesh, in_specs=(tokens, P(None), whole, whole, whole, whole), out_specs=tokens, check_vma=False)
```

```python
import functools

import jax
import jax.numpy as jnp
import numpy as np
from jax import lax
from jax.experimental import pallas as pl
from jax.experimental.pallas import tpu as pltpu
from jax.sharding import PartitionSpec as P

HEAD = 256
THETA = 10000
LOG2E = 1.4426950408889634
HIDDEN = -1e30
MESH = pl.DeviceIdType.MESH
F32, BF16 = jnp.float32, jnp.bfloat16
WKV, WQ, KV, WO = range(4)

STAGES = (
    ((0, 0),),
    ((1, 0), (0, 1), (0, 2)),
    ((2, 0), (1, 1), (1, 2), (0, 3)),
    ((3, 0), (2, 1), (2, 2), (1, 3)),
    ((3, 1), (3, 2), (2, 3)),
    ((3, 3),),
)
MAIN, A, B, LATE, LATE_A, LATE_B = range(6)
CUTS = {
    WKV: (1, ((0, 512), (0, 256), (256, 256), None, None, None)),
    WQ: (1, ((0, 1408), (0, 640), (640, 768), (1408, 640), (1408, 384), (1792, 256))),
    KV: (0, ((0, 400), (0, 192), (192, 208), (400, 112), (400, 64), (464, 48))),
    WO: (1, ((0, 1792), (0, 896), (896, 896), (1792, 256), (1792, 128), (1920, 128))),
}


WORK = {1: ((KV, 3),), 3: ((WO, 2),), 7: ((KV, 4),), 10: ((WO, 3),), 11: ((KV, 5),), 14: ((WO, 4),)}


def dot(a, b):
    return jnp.dot(a, b, preferred_element_type=F32)


def kernel(x_hbm, gain_hbm, freq_hbm, wq_ref, wk_ref, wv_ref, wo_ref, out_hbm,
           wqb, wob, wkvb, kvb, x_ref, gain_ref, freq_ref, out_ref, a_s, qt_s, mix_s, acc_s, top_s, cos_s, sin_s,
           local_sem, out_sem, up_s, down_s, z_r, x_s, x_r, y_s, y_r, ha_s, ha_r, hb_s, hb_r, p_s, p_r,
           late_s, late_r, late_up_s, late_down_s, late_z_r, late_p_s, late_p_r):
    me = lax.axis_index("sp")
    core, chip = lax.rem(me, 2), lax.div(me, 2)
    z, y, x = lax.rem(chip, 4), lax.rem(lax.div(chip, 4), 2), lax.div(chip, 8)
    ranks = (z, z + 1 - 2 * lax.rem(z, 2), jnp.where(z >= 2, 1, 2), jnp.where(z >= 2, 0, 3))
    columns = (x * 2 + y, x * 2 + 1 - y, (1 - x) * 2 + y, (1 - x) * 2 + 1 - y)
    above, below, partner = me + 2, me - 2, me + 1 - 2 * core
    x_peer, y_peer = columns[2] * 8 + z * 2 + core, columns[1] * 8 + z * 2 + core
    bufs = (wkvb, wqb, kvb, wob)

    def remote(src, send_sem, recv_sem, to):
        return pltpu.make_async_remote_copy(src_ref=src, dst_ref=src, send_sem=send_sem, recv_sem=recv_sem, device_id={"sp": to}, device_id_type=MESH)

    def given(when, do):
        if when is None:
            do()
        else:
            pl.when(when)(do)

    def arrived(ref, recv_sem):
        pltpu.make_async_remote_copy(src_ref=ref, dst_ref=ref, send_sem=recv_sem, recv_sem=recv_sem, device_id={"sp": partner}, device_id_type=MESH).wait_recv()

    def piece(u, r, q, c, which):
        axis, cuts = CUTS[u]
        start, size = cuts[which]
        column = slice(None) if q is None else columns[q]
        here = pl.ds(start, size)
        return bufs[u].at[column, ranks[r], c, here] if axis == 0 else bufs[u].at[column, ranks[r], c, :, here]

    def sends(u, r, q):
        ref = piece(u, r, q, core, MAIN)
        copies = [(remote(ref, p_s.at[u, 4 * q + r], p_r.at[u, 4 * q + r], partner), None)]
        if q == 0:
            at = ranks[r]
            copies = [
                (remote(ref, up_s.at[u, r], z_r.at[u, at], above), (at <= z) & (z < 3)),
                (remote(ref, down_s.at[u, r], z_r.at[u, at], below), (at >= z) & (z > 0)),
                (remote(ref, x_s.at[u, r], x_r.at[u, r], x_peer), None),
                (remote(ref, y_s.at[u, r], y_r.at[u, r], y_peer), None),
            ] + copies
        elif q == 1:
            copies = [(remote(piece(u, r, q, core, B), hb_s.at[u, r], hb_r.at[u, r], x_peer), None)] + copies
        elif q == 2:
            copies = [(remote(piece(u, r, q, core, A), ha_s.at[u, r], ha_r.at[u, r], y_peer), None)] + copies
        return copies

    def event(u, r, q):
        if q == 0 and r:
            arrived(piece(u, r, q, core, MAIN), z_r.at[u, ranks[r]])
        elif q == 1:
            arrived(piece(u, r, q, core, MAIN), y_r.at[u, r])
        elif q == 2:
            arrived(piece(u, r, q, core, MAIN), x_r.at[u, r])
        elif q == 3:
            arrived(piece(u, r, q, core, A), ha_r.at[u, r])
            arrived(piece(u, r, q, core, B), hb_r.at[u, r])
        for copy, when in sends(u, r, q):
            given(when, copy.start)

    def late_sends(u, n):
        if n == 0:
            ref = piece(u, 0, 0, core, LATE)
            return [(remote(ref, late_s.at[u, 0], late_r.at[u, 0], x_peer), None), (remote(ref, late_s.at[u, 1], late_r.at[u, 1], y_peer), None)]
        if n == 1:
            copies = [(remote(piece(u, 0, 2, core, LATE_A), late_s.at[u, 2], late_r.at[u, 2], y_peer), None)]
            if CUTS[u][1][LATE_B]:
                copies.append((remote(piece(u, 0, 1, core, LATE_B), late_s.at[u, 3], late_r.at[u, 3], x_peer), None))
            return copies
        r = n - 2
        at, ref = ranks[r], piece(u, r, None, core, LATE)
        return [
            (remote(ref, late_up_s.at[u, r], late_z_r.at[u, at], above), (at <= z) & (z < 3)),
            (remote(ref, late_down_s.at[u, r], late_z_r.at[u, at], below), (at >= z) & (z > 0)),
            (remote(ref, late_p_s.at[u, r], late_p_r.at[u, r], partner), None),
        ]

    def late_event(u, n):
        if n == 1:
            arrived(piece(u, 0, 2, core, LATE), late_r.at[u, 0])
            arrived(piece(u, 0, 1, core, LATE), late_r.at[u, 1])
        elif n == 2:
            arrived(piece(u, 0, 3, core, LATE_A), late_r.at[u, 2])
            if CUTS[u][1][LATE_B]:
                arrived(piece(u, 0, 3, core, LATE_B), late_r.at[u, 3])
        elif n > 2:
            arrived(piece(u, n - 2, None, core, LATE), late_z_r.at[u, ranks[n - 2]])
        for copy, when in late_sends(u, n):
            given(when, copy.start)

    def stage(u, n):
        if u != WKV and n < 5:
            late_event(u, n)
        for r, q in STAGES[n]:
            event(u, r, q)
        if u != WKV and not n < 5:
            late_event(u, n)

    def other(u, r, q):
        arrived(piece(u, r, q, 1 - core, MAIN), p_r.at[u, 4 * q + r])
        if u != WKV and q == 0:
            arrived(piece(u, r, None, 1 - core, LATE), late_p_r.at[u, r])

    def others(u):
        for r in range(4):
            for q in range(4):
                other(u, r, q)

    own = [
        pltpu.make_async_copy(wk_ref, wkvb.at[columns[0], z, core, :, pl.ds(0, HEAD)], local_sem.at[0]),
        pltpu.make_async_copy(wv_ref, wkvb.at[columns[0], z, core, :, pl.ds(HEAD, HEAD)], local_sem.at[1]),
        pltpu.make_async_copy(wq_ref, wqb.at[columns[0], z, core], local_sem.at[2]),
        pltpu.make_async_copy(wo_ref, wob.at[columns[0], z, core], local_sem.at[3]),
        pltpu.make_async_copy(x_hbm, x_ref, local_sem.at[4]),
        pltpu.make_async_copy(gain_hbm, gain_ref, local_sem.at[5]),
        pltpu.make_async_copy(freq_hbm, freq_ref, local_sem.at[6]),
    ]

    barrier = pltpu.get_barrier_semaphore()

    def greet(to):
        pl.semaphore_signal(barrier, inc=1, device_id={"sp": to}, device_id_type=MESH)

    for to in (x_peer, y_peer, partner):
        greet(to)
    pl.when(z < 3)(lambda: greet(above))
    pl.when(z > 0)(lambda: greet(below))
    for copy in own:
        copy.start()
    pl.semaphore_wait(barrier, jnp.where((z > 0) & (z < 3), 5, 4))

    rows, wide = x_ref.shape
    heads = wide // HEAD

    def normalise():
        for copy in own[4:]:
            copy.wait()
        gain = gain_ref[...].astype(F32).reshape(1, -1)

        @pl.loop(0, rows // 64)
        def _(n):
            here = pl.ds(n * 64, 64)
            wide = x_ref[here, :].astype(F32)
            scale = lax.rsqrt(jnp.mean(wide * wide, -1, keepdims=True) + 1e-6)
            a = (wide * scale * gain).astype(BF16)
            for i in range(16):
                a_s[i // 4, i % 4, here, :] = a[:, i * 128 : (i + 1) * 128]

        place = (me * rows + lax.broadcasted_iota(jnp.int32, (rows, HEAD // 2), 0)).astype(F32)
        angle = place * freq_ref[...]
        cos_s[...] = jnp.cos(angle)
        sin_s[...] = jnp.sin(angle)

    def turned(t):
        t = t.astype(BF16).astype(F32)
        a, b, cos, sin = t[:, : HEAD // 2], t[:, HEAD // 2 :], cos_s[...], sin_s[...]
        return jnp.concatenate([a * cos - b * sin, b * cos + a * sin], -1)

    def strip_of(ref, ranks_in):
        return jnp.concatenate([ref[q, r] for r in ranks_in for q in range(4)], axis=1)

    def partial(ref, weights, ranks_in, into, first):
        left = strip_of(ref, ranks_in)

        @pl.loop(0, wide // 512)
        def _(n):
            cols = pl.ds(pl.multiple_of(n * 512, 512), 512)
            right = jnp.concatenate([weights[:, r, :, :, cols].reshape(-1, 512) for r in ranks_in], axis=0)
            got = dot(left, right)
            into[0:rows, cols] = got if first else into[0:rows, cols] + got

    def rank_in(u, r):
        for q in range(4):
            other(u, r, q)

    def query(n, first=False):
        rank_in(WQ, n)
        partial(a_s, wqb, [ranks[n]], mix_s, first)

    def keys_values():
        others(WKV)
        kv = dot(strip_of(a_s, range(4)), jnp.concatenate([wkvb[:, r].reshape(-1, 2 * HEAD) for r in range(4)], axis=0))
        kvb[columns[0], z, core, 0:HEAD, :] = turned(kv[:, :HEAD]).astype(BF16)
        kvb[columns[0], z, core, HEAD:, :] = kv[:, HEAD:].astype(BF16).astype(F32).T.astype(BF16)

    def queries_turned():
        @pl.loop(0, heads)
        def _(h):
            cols = pl.ds(pl.multiple_of(h * HEAD, HEAD), HEAD)
            qt_s[:, cols] = turned(mix_s[0:rows, cols]).T.astype(BF16)

    own[0].wait()
    own[1].wait()
    stage(WKV, 0)
    normalise()
    own[2].wait()
    stage(WQ, 0)
    for u, n in ((WKV, 1), (WKV, 2), (WKV, 3), (WQ, 1)):
        stage(u, n)
    own[3].wait()
    for u, n in ((WO, 0), (WKV, 4), (WQ, 2), (WKV, 5)):
        stage(u, n)
    keys_values()
    stage(KV, 0)
    query(0, True)
    for u, n in ((WQ, 3), (KV, 1), (WQ, 4), (KV, 2), (WO, 1)):
        stage(u, n)
    query(1)
    stage(WQ, 5)
    query(2)
    query(3)
    queries_turned()

    e = HEAD**-0.5 * LOG2E
    width = qt_s.shape[1]
    strip = 512
    strips = range(0, width, strip)
    keys = 2 * rows
    ones = jnp.ones((8, keys), BF16)

    def step(column, at, masked):
        k = kvb[column, at, :, 0:HEAD, :].reshape(keys, HEAD)
        v = jnp.concatenate([kvb[column, at, 0, HEAD:, :], kvb[column, at, 1, HEAD:, :]], axis=1)
        v = jnp.concatenate([v, ones], axis=0)
        scores = [dot(k, qt_s[:, n : n + strip]) for n in strips]
        weights, keeps = [], []
        for n, s in zip(strips, scores):
            if masked:
                ahead = lax.rem(lax.broadcasted_iota(jnp.int32, s.shape, 1), rows) - lax.broadcasted_iota(jnp.int32, s.shape, 0)
                s = jnp.where(ahead >= -rows * core, s, HIDDEN)
                top = s.max(axis=0, keepdims=True)
            else:
                old = top_s[0:1, n : n + strip]
                top = jnp.maximum(old, s.max(axis=0, keepdims=True))
                keeps.append(jnp.exp2((old - top) * e))
            top_s[0:1, n : n + strip] = top
            weights.append(jnp.exp2((s - top) * e).astype(BF16))
        for i, n in enumerate(strips):
            add = dot(v, weights[i])
            mix_s[:, n : n + strip] = add if masked else mix_s[:, n : n + strip] * keeps[i] + add

    other(KV, 0, 0)
    step(columns[0], z, True)

    @pl.loop(1, 16)
    def _(i):
        def at(n, *todo):
            @pl.when(i == n)
            def _():
                for do in todo:
                    do()

        for r in range(4):
            for q in range(4):
                n = 4 * r + q
                todo = []
                for u, m in WORK.get(n, ()):
                    todo.append(functools.partial(stage, u, m))
                if n:
                    todo.append(functools.partial(other, KV, r, q))
                    at(n, *todo)

        r, q = lax.div(i, 4), lax.rem(i, 4)
        rank = jnp.where(r == 0, ranks[0], jnp.where(r == 1, ranks[1], jnp.where(r == 2, ranks[2], ranks[3])))
        column = jnp.where(q == 0, columns[0], jnp.where(q == 1, columns[1], jnp.where(q == 2, columns[2], columns[3])))

        @pl.when(column * 4 + rank < chip)
        def _():
            step(column, rank, False)

    def attended():
        @pl.loop(0, heads)
        def _(h):
            cols = pl.ds(pl.multiple_of(h * HEAD, HEAD), HEAD)
            o = (mix_s[0:HEAD, cols] * (1 / mix_s[HEAD : HEAD + 1, cols])).T.astype(BF16)
            column, at = lax.div(h, 2), 2 * lax.rem(h, 2)
            a_s[column, at] = o[:, : HEAD // 2]
            a_s[column, at + 1] = o[:, HEAD // 2 :]

    stores = []

    def finish(left, ranks_in, start, first, last):
        for n in range(start, start + 1024, 512):
            cols = pl.ds(n, 512)
            got = dot(left, jnp.concatenate([wob[:, r, :, :, cols].reshape(-1, 512) for r in ranks_in], axis=0))
            if not first:
                got = acc_s[:, cols] + got
            if last:
                out_ref[:, cols] = (x_ref[:, cols].astype(F32) + got).astype(BF16)
                stores.append(pltpu.make_async_copy(out_ref.at[:, cols], out_hbm.at[:, cols], out_sem.at[len(stores)]))
                stores[-1].start()
            else:
                acc_s[:, cols] = got

    for u in (WKV, WQ):
        copies = [copy for r in range(4) for q in range(4) for copy in sends(u, r, q)]
        if u != WKV:
            copies += [copy for n in range(6) for copy in late_sends(u, n)]
        for copy, when in copies:
            given(when, copy.wait_send)
    attended()
    stage(WO, 5)
    for r in range(3):
        rank_in(WO, r)
    for at in (0, 1024):
        finish(strip_of(a_s, ranks[:3]), ranks[:3], at, True, False)
    rank_in(WO, 3)
    for at in (0, 1024):
        finish(strip_of(a_s, ranks[3:]), ranks[3:], at, False, True)
    for copy in stores:
        copy.wait()

    for u in (KV, WO):
        copies = [copy for r in range(4) for q in range(4) for copy in sends(u, r, q)]
        if u != WKV:
            copies += [copy for n in range(6) for copy in late_sends(u, n)]
        for copy, when in copies:
            given(when, copy.wait_send)


def solution(mesh):
    half = HEAD // 2
    freq = (float(THETA) ** (-np.arange(half, dtype=np.float64) / half)).astype(np.float32)[None]

    def step(x, gain, wq, wk, wv, wo):
        rows, wide = x.shape
        deep, width = wq.shape
        hbm = pl.BlockSpec(memory_space=pltpu.HBM)
        dma = pltpu.SemaphoreType.DMA
        return pl.pallas_call(
            kernel,
            out_shape=jax.ShapeDtypeStruct((rows, wide), BF16),
            in_specs=[hbm] * 7,
            out_specs=hbm,
            scratch_shapes=[
                pltpu.VMEM((4, 4, 2, deep, width), BF16),
                pltpu.VMEM((4, 4, 2, deep, wide), BF16),
                pltpu.VMEM((4, 4, 2, deep, 2 * HEAD), BF16),
                pltpu.VMEM((4, 4, 2, 2 * HEAD, HEAD), BF16),
                pltpu.VMEM((rows, wide), BF16),
                pltpu.VMEM((wide,), BF16),
                pltpu.VMEM((1, half), F32),
                pltpu.VMEM((rows, wide), BF16),
                pltpu.VMEM((4, 4, rows, 2 * deep), BF16),
                pltpu.VMEM((HEAD, width), BF16),
                pltpu.VMEM((HEAD + 8, width), F32),
                pltpu.VMEM((rows, wide), F32),
                pltpu.VMEM((8, width), F32),
                pltpu.VMEM((rows, half), F32),
                pltpu.VMEM((rows, half), F32),
                dma((7,)),
                dma((4,)),
                *[dma((4, 4))] * 11,
                *[dma((4, 16))] * 2,
                *[dma((4, 4))] * 7,
            ],
            compiler_params=pltpu.CompilerParams(collective_id=0, has_side_effects=True, vmem_limit_bytes=63 * 2**20),
        )(x, gain, jnp.asarray(freq), wq, wk, wv, wo)

    tokens, whole = P(("dp", "sp"), None), P("sp", None)
    return jax.shard_map(step, mesh=mesh, in_specs=(tokens, P(None), whole, whole, whole, whole), out_specs=tokens, check_vma=False)
```
